32 devices in a mesh: trial: 4 (over z), span: 4 (over y, core), heads: 2 (over x).
Axes of the slice: x: 2, y: 2, z: 4, core: 2. Of those that a mesh axis runs over, the one named last changes fastest.
Arguments:
- latents: bfloat16 [16, 1024, 512], P('trial', ('span', 'heads')), parts along dimension 0, may hold values from -6 to 6
- rotary_rows: bfloat16 [16, 1024, 64], P('trial', ('span', 'heads')), parts along dimension 0, may hold values from -6 to 6
- latent_gain: float32 [512], replicated, may hold values from 0.25 to 1.75
- key_up: bfloat16 [2048, 16, 128], P('trial', 'heads'), parts along dimension 0, may hold values from -0.25 to 0.25
- value_up: bfloat16 [2048, 16, 128], P('trial', 'heads'), parts along dimension 0, may hold values from -0.25 to 0.25
Outputs:
- cache_keys: bfloat16 [16, 16, 192, 1024], P(('trial', 'span'), 'heads'), parts along dimension 0
- cache_values: bfloat16 [16, 1024, 16, 128], P(('trial', 'span'), None, 'heads'), parts along dimension 0
The draws below stay inside these ranges and needn't reach their ends.
There are 4 independent parts, one for each index of `trial`. The reference program is written for one: setup_inputs(seed, part) draws one part's arguments, and reference() takes and returns one part's arrays. A program takes and returns all parts, laid end to end along the dimension named above; an argument that names none is the same for every part. Nothing has to cross between parts.
All inputs are finite; a program needn't handle non-finite values.
Results may differ from the reference program's by a relative error of at most 0.0049.
Values may be sent and summed in bfloat16 or wider, within the bound.
A program may use at most 64 MiB of HBM per device.

```python
import jax
import jax.numpy as jnp
from jax import lax

BATCH = 4
LENGTH = 1024
HEADS = 16
LATENT = 512
KEY_PART = 128
ROTARY = 64
VALUE_SIZE = 128


def shard_levels(key, extent, shards, smallest, high):
    level, own = 1.0, jax.random.fold_in(key, 6)
    for dim, blocks in shards:
        steps = jnp.exp(jax.random.uniform(jax.random.fold_in(own, dim), (blocks,), jnp.float32, smallest / len(shards), high / len(shards)))
        level = level * jnp.repeat(steps, extent[dim] // blocks).reshape([-1 if axis == dim else 1 for axis in range(len(extent))])
    return level


def bell_draw(own_key, shape, width, most, cuts=(), kind=jnp.bfloat16):
    values = width * jax.random.normal(own_key, shape, jnp.float32)
    if cuts:
        values = values * shard_levels(own_key, shape, cuts, -0.22, 0.18)
    return jnp.clip(values, -most, most).astype(kind)


def setup_inputs(seed: int = 0, part: int = 0) -> dict:
    seeds = jax.random.split(jax.random.key(seed), 6)
    own_keys = jax.random.split(jax.random.fold_in(seeds[5], part), 6)
    return {
        "latents": bell_draw(own_keys[0], (BATCH, LENGTH, LATENT), 1.0, 6.0, ((1, 8),)),
        "rotary_rows": bell_draw(own_keys[1], (BATCH, LENGTH, ROTARY), 1.0, 6.0, ((1, 8),)),
        "latent_gain": jnp.clip(1.0 + 0.15 * jax.random.normal(seeds[2], (LATENT,), jnp.float32), 0.25, 1.75),
        "key_up": bell_draw(own_keys[3], (LATENT, HEADS, KEY_PART), LATENT ** -0.5, 0.25, ((1, 2),)),
        "value_up": bell_draw(own_keys[4], (LATENT, HEADS, VALUE_SIZE), LATENT ** -0.5, 0.25, ((1, 2),)),
    }


def unit_rows(vectors, row_gain):
    return vectors * lax.rsqrt(lax.optimization_barrier(jnp.mean(vectors * vectors, axis=-1, keepdims=True)) + 1e-06) * row_gain

def reference(latents, rotary_rows, latent_gain, key_up, value_up):
    rows_ready = unit_rows(latents.astype(jnp.float32), latent_gain).astype(jnp.bfloat16)
    rows_ready = lax.optimization_barrier(rows_ready)

    def expand_one(one):
        rows_one, rotary_one = one
        wide_keys = jnp.einsum('tr,rhk->thk', rows_one.astype(jnp.float32), key_up.astype(jnp.float32)).astype(jnp.bfloat16)
        shared = jnp.broadcast_to(rotary_one[:, None], (LENGTH, HEADS, ROTARY))
        wide_values = jnp.einsum('tr,rhk->thk', rows_one.astype(jnp.float32), value_up.astype(jnp.float32)).astype(jnp.bfloat16)
        return (jnp.concatenate([wide_keys, shared], axis=-1), wide_values)
    cache_keys, cache_values = lax.map(expand_one, (rows_ready, rotary_rows))
    cache_keys = jnp.transpose(cache_keys, (0, 2, 3, 1))
    return (cache_keys, cache_values)
```

```python
import functools

import jax
import jax.numpy as jnp
from jax import lax
from jax.experimental import pallas as pl
from jax.experimental.pallas import tpu as pltpu
from jax.sharding import PartitionSpec as P

MESH = pl.DeviceIdType.MESH


def widen_rows(rows, rotary, key_up, value_up):
    wide_keys = jnp.einsum(
        "btr,rhk->bthk", rows, key_up, preferred_element_type=jnp.float32
    ).astype(jnp.bfloat16)
    shared = jnp.broadcast_to(rotary[:, :, None], wide_keys.shape[:3] + rotary.shape[2:])
    wide_values = jnp.einsum(
        "btr,rhk->bthk", rows, value_up, preferred_element_type=jnp.float32
    ).astype(jnp.bfloat16)
    return (jnp.concatenate([wide_keys, shared], axis=-1), wide_values)


def unit_rows(vectors, row_gain):
    return (
        vectors * lax.rsqrt(jnp.mean(vectors * vectors, axis=-1, keepdims=True) + 1e-06) * row_gain
    )


def plain_shards(latents, rotary_rows, latent_gain, key_up, value_up):
    rows_ready = unit_rows(latents.astype(jnp.float32), latent_gain).astype(jnp.bfloat16)

    def move(block):
        block = lax.all_to_all(block, "span", split_axis=0, concat_axis=1, tiled=True)
        block = block.reshape(block.shape[0], lax.axis_size("span"), -1, block.shape[2])
        block = lax.all_gather(block, "heads", axis=2, tiled=True)
        return block.reshape(block.shape[0], -1, block.shape[3])

    cache_keys, cache_values = widen_rows(move(rows_ready), move(rotary_rows), key_up, value_up)
    return (jnp.transpose(cache_keys, (0, 2, 3, 1)), cache_values)


def exchange_kernel(
    spans, lat, rot, gain, key_up, value_up, keys, values,
    stage, stage_rot, rows, turned, raw_key, raw_value, key_wide, value_wide, flat, flat_out,
    load_sem, weight_sem, send_sem, recv_sem, pass_sem, land_sem,
):
    me, side = lax.axis_index("span"), lax.axis_index("heads")
    other = 1 - side
    count, depth = lat.shape[1], lat.shape[2]
    heads, width = key_up.shape[1], key_up.shape[2]
    value_width = value_up.shape[2]
    turn = rot.shape[1]
    both = 2 * count

    def sibling(p):
        return p + 1 - 2 * lax.rem(p, 2)

    targets, sources = [sibling(me)], [sibling(me)]
    for j in range(1, spans // 2):
        ahead, behind = lax.rem(me + 2 * j, spans), lax.rem(me + spans - 2 * j, spans)
        targets += [ahead, sibling(ahead)]
        sources += [behind, lax.rem(sibling(me) + spans - 2 * j, spans)]
    steps = len(targets)

    barrier = pltpu.get_barrier_semaphore()
    for q in targets:
        pl.semaphore_signal(barrier, inc=1, device_id={"span": q}, device_id_type=MESH)
    pl.semaphore_signal(barrier, inc=1, device_id={"heads": other}, device_id_type=MESH)

    order = list(range(1, steps)) + [0]
    loads = {}
    own = (
        pltpu.make_async_copy(lat.at[me], rows.at[me, side], load_sem.at[0, steps]),
        pltpu.make_async_copy(rot.at[me], turned.at[me, side], load_sem.at[1, steps]),
    )
    for copy in own:
        copy.start()
    for i in order:
        loads[i] = (
            pltpu.make_async_copy(lat.at[targets[i]], stage.at[i], load_sem.at[0, i]),
            pltpu.make_async_copy(rot.at[targets[i]], stage_rot.at[i], load_sem.at[1, i]),
        )
        for copy in loads[i]:
            copy.start()
    weights = (
        pltpu.make_async_copy(key_up, raw_key, weight_sem.at[0]),
        pltpu.make_async_copy(value_up, raw_value, weight_sem.at[1]),
    )
    for copy in weights:
        copy.start()
    pl.semaphore_wait(barrier, steps + 1)

    def forward(q, i):
        made = []
        for k, held in enumerate((rows, turned)):
            made.append(pltpu.make_async_remote_copy(
                src_ref=held.at[q, side], dst_ref=held.at[q, side],
                send_sem=pass_sem.at[k, i], recv_sem=land_sem.at[k, i],
                device_id={"heads": other}, device_id_type=MESH,
            ))
            made[-1].start()
        return made

    for copy in own:
        copy.wait()
    passed = [forward(me, 0)]
    sent = {}
    for i in order:
        for copy in loads[i]:
            copy.wait()
        sent[i] = []
        for k, (held, land) in enumerate(((stage, rows), (stage_rot, turned))):
            sent[i].append(pltpu.make_async_remote_copy(
                src_ref=held.at[i], dst_ref=land.at[me, side],
                send_sem=send_sem.at[k, i], recv_sem=recv_sem.at[k, i],
                device_id={"span": targets[i]}, device_id_type=MESH,
            ))
            sent[i][-1].start()

    def hear(i):
        for k, (held, land) in enumerate(((stage, rows), (stage_rot, turned))):
            pltpu.make_async_remote_copy(
                src_ref=held.at[i], dst_ref=land.at[sources[i], side],
                send_sem=send_sem.at[k, i], recv_sem=recv_sem.at[k, i],
                device_id={"span": targets[i]}, device_id_type=MESH,
            ).wait_recv()
        passed.append(forward(sources[i], i + 1))

    def landed(q, i):
        for k, held in enumerate((rows, turned)):
            pltpu.make_async_remote_copy(
                src_ref=held.at[q, other], dst_ref=held.at[q, other],
                send_sem=pass_sem.at[k, i], recv_sem=land_sem.at[k, i],
                device_id={"heads": other}, device_id_type=MESH,
            ).wait_recv()

    def unravel(raw, size, put):
        piece = 128

        @pl.loop(0, depth // piece)
        def _(n):
            r = pl.multiple_of(n * piece, piece)
            part = raw[pl.ds(r, piece)].astype(jnp.float32)
            flat[pl.ds(0, piece * heads), :] = part.reshape(piece * heads, size)
            for h in range(heads):
                put(h, r, piece, flat[pl.ds(h, piece, stride=heads), :])

    def put_value(h, r, piece, block):
        value_wide[pl.ds(r, piece), h * value_width:(h + 1) * value_width] = block.astype(jnp.bfloat16)

    def put_key(h, r, piece, block):
        key_wide[h * width:(h + 1) * width, pl.ds(r, piece)] = block.T.astype(jnp.bfloat16)

    def expand(q):
        raw = rows[q].reshape(both, depth).astype(jnp.float32)
        ready = unit_rows(raw, gain[...]).astype(jnp.bfloat16)
        start = pl.multiple_of(q * both, both)
        for h in range(heads):
            wide = lax.dot_general(
                key_wide[h * width:(h + 1) * width, :], ready,
                (((1,), (1,)), ((), ())), preferred_element_type=jnp.float32,
            )
            keys[0, h, :width, pl.ds(start, both)] = wide.astype(jnp.bfloat16)
            for k in range(2):
                keys[0, h, width:width + turn, pl.ds(start + k * count, count)] = turned[q, k]
        pair = 2 * value_width
        for h in range(0, heads, 2):
            wide = jnp.dot(
                ready, value_wide[:, h * value_width:h * value_width + pair],
                preferred_element_type=jnp.float32,
            )
            for k in range(2):
                flat_out[pl.ds(h + k, both, stride=heads), :] = wide[:, k * value_width:(k + 1) * value_width]
        values[0, pl.ds(start, both)] = flat_out[...].reshape(both, heads, value_width).astype(jnp.bfloat16)

    hear(0)
    for copy in weights:
        copy.wait()
    unravel(raw_key, width, put_key)
    unravel(raw_value, value_width, put_value)
    for i in range(1, steps):
        hear(i)
        landed((me, *sources)[i - 1], i - 1)
        expand((me, *sources)[i - 1])
    for i in range(steps - 1, steps + 1):
        landed((me, *sources)[i], i)
        expand((me, *sources)[i])
    for pair in (*passed, *sent.values()):
        for copy in pair:
            copy.wait_send()


def shards(latents, rotary_rows, latent_gain, key_up, value_up):
    spans, sides = lax.axis_size("span"), lax.axis_size("heads")
    _, count, depth = latents.shape
    turn = rotary_rows.shape[2]
    heads, width, value_width = key_up.shape[1], key_up.shape[2], value_up.shape[2]
    if (
        latents.shape[0] != spans or spans % 2 or sides != 2 or count % 128 or depth % 128
        or heads % 8 or width != 128 or value_width != 128 or turn % 16
    ):
        return plain_shards(latents, rotary_rows, latent_gain, key_up, value_up)
    length = spans * sides * count
    anywhere = pl.BlockSpec(memory_space=pl.ANY)
    steps = spans - 1
    bf16 = jnp.bfloat16
    keys, values = pl.pallas_call(
        functools.partial(exchange_kernel, spans),
        out_shape=(
            jax.ShapeDtypeStruct((1, heads, width + turn, length), bf16),
            jax.ShapeDtypeStruct((1, length, heads, value_width), bf16),
        ),
        in_specs=[anywhere, anywhere, pl.BlockSpec(memory_space=pltpu.VMEM), anywhere, anywhere],
        out_specs=[pl.BlockSpec(memory_space=pltpu.VMEM)] * 2,
        scratch_shapes=[
            pltpu.VMEM((steps, count, depth), bf16),
            pltpu.VMEM((steps, turn, count), bf16),
            pltpu.VMEM((spans, sides, count, depth), bf16),
            pltpu.VMEM((spans, sides, turn, count), bf16),
            pltpu.VMEM(key_up.shape, bf16),
            pltpu.VMEM(value_up.shape, bf16),
            pltpu.VMEM((heads * width, depth), bf16),
            pltpu.VMEM((depth, heads * value_width), bf16),
            pltpu.VMEM((128 * heads, 128), jnp.float32),
            pltpu.VMEM((2 * count * heads, value_width), jnp.float32),
            pltpu.SemaphoreType.DMA((2, spans)),
            pltpu.SemaphoreType.DMA((2,)),
            pltpu.SemaphoreType.DMA((2, steps)),
            pltpu.SemaphoreType.DMA((2, steps)),
            pltpu.SemaphoreType.DMA((2, spans)),
            pltpu.SemaphoreType.DMA((2, spans)),
        ],
        compiler_params=pltpu.CompilerParams(
            collective_id=0, has_side_effects=True, vmem_limit_bytes=40 * 1024 * 1024
        ),
    )(latents, jnp.swapaxes(rotary_rows, 1, 2), latent_gain[None], key_up, value_up)
    return keys, values


def solution(mesh):
    return jax.shard_map(
        shards,
        mesh=mesh,
        in_specs=(
            P("trial", ("span", "heads"), None),
            P("trial", ("span", "heads"), None),
            P(),
            P("trial", "heads", None),
            P("trial", "heads", None),
        ),
        out_specs=(
            P(("trial", "span"), "heads", None, None),
            P(("trial", "span"), None, "heads", None),
        ),
        check_vma=False,
    )
```

```python
import functools

import jax
import jax.numpy as jnp
from jax import lax
from jax.experimental import pallas as pl
from jax.experimental.pallas import tpu as pltpu
from jax.sharding import PartitionSpec as P

MESH = pl.DeviceIdType.MESH


def widen_rows(rows, rotary, key_up, value_up):
    wide_keys = jnp.einsum(
        "btr,rhk->bthk", rows, key_up, preferred_element_type=jnp.float32
    ).astype(jnp.bfloat16)
    shared = jnp.broadcast_to(rotary[:, :, None], wide_keys.shape[:3] + rotary.shape[2:])
    wide_values = jnp.einsum(
        "btr,rhk->bthk", rows, value_up, preferred_element_type=jnp.float32
    ).astype(jnp.bfloat16)
    return (jnp.concatenate([wide_keys, shared], axis=-1), wide_values)


def unit_rows(vectors, row_gain):
    return (
        vectors * lax.rsqrt(jnp.mean(vectors * vectors, axis=-1, keepdims=True) + 1e-06) * row_gain
    )


def plain_shards(latents, rotary_rows, latent_gain, key_up, value_up):
    rows_ready = unit_rows(latents.astype(jnp.float32), latent_gain).astype(jnp.bfloat16)

    def move(block):
        block = lax.all_to_all(block, "span", split_axis=0, concat_axis=1, tiled=True)
        block = block.reshape(block.shape[0], lax.axis_size("span"), -1, block.shape[2])
        block = lax.all_gather(block, "heads", axis=2, tiled=True)
        return block.reshape(block.shape[0], -1, block.shape[3])

    cache_keys, cache_values = widen_rows(move(rows_ready), move(rotary_rows), key_up, value_up)
    return (jnp.transpose(cache_keys, (0, 2, 3, 1)), cache_values)


def exchange_kernel(
    spans, lat, rot, far_gain, key_up, value_up, keys, values,
    gain, stage, stage_rot, rows, turned, raw_key, raw_value, key_wide, value_wide, flat, flat_out,
    load_sem, weight_sem, send_sem, recv_sem, pass_sem, land_sem,
):
    me, side = lax.axis_index("span"), lax.axis_index("heads")
    other = 1 - side
    count, depth = lat.shape[1], lat.shape[2]
    heads, width = key_up.shape[1], key_up.shape[2]
    value_width = value_up.shape[2]
    turn = rot.shape[1]
    both = 2 * count

    def sibling(p):
        return p + 1 - 2 * lax.rem(p, 2)

    targets, sources = [sibling(me)], [sibling(me)]
    for j in range(1, spans // 2):
        ahead, behind = lax.rem(me + 2 * j, spans), lax.rem(me + spans - 2 * j, spans)
        targets += [ahead, sibling(ahead)]
        sources += [behind, lax.rem(sibling(me) + spans - 2 * j, spans)]
    steps = len(targets)

    barrier = pltpu.get_barrier_semaphore()
    for q in targets:
        pl.semaphore_signal(barrier, inc=1, device_id={"span": q}, device_id_type=MESH)
    pl.semaphore_signal(barrier, inc=1, device_id={"heads": other}, device_id_type=MESH)

    order = list(range(1, steps)) + [0]
    loads = {}
    own = (
        pltpu.make_async_copy(lat.at[me], rows.at[me, side], load_sem.at[0, steps]),
        pltpu.make_async_copy(rot.at[me], turned.at[me, side], load_sem.at[1, steps]),
    )
    for copy in own:
        copy.start()
    for i in order:
        loads[i] = (
            pltpu.make_async_copy(lat.at[targets[i]], stage.at[i], load_sem.at[0, i]),
            pltpu.make_async_copy(rot.at[targets[i]], stage_rot.at[i], load_sem.at[1, i]),
        )
        for copy in loads[i]:
            copy.start()
    weights = (
        pltpu.make_async_copy(key_up, raw_key, weight_sem.at[0]),
        pltpu.make_async_copy(value_up, raw_value, weight_sem.at[1]),
        pltpu.make_async_copy(far_gain, gain, weight_sem.at[2]),
    )
    for copy in weights:
        copy.start()
    pl.semaphore_wait(barrier, steps + 1)

    def forward(q, i):
        made = []
        for k, held in enumerate((rows, turned)):
            made.append(pltpu.make_async_remote_copy(
                src_ref=held.at[q, side], dst_ref=held.at[q, side],
                send_sem=pass_sem.at[k, i], recv_sem=land_sem.at[k, i],
                device_id={"heads": other}, device_id_type=MESH,
            ))
            made[-1].start()
        return made

    for copy in own:
        copy.wait()
    passed = [forward(me, 0)]
    sent = {}
    for i in order:
        for copy in loads[i]:
            copy.wait()
        sent[i] = []
        for k, (held, land) in enumerate(((stage, rows), (stage_rot, turned))):
            sent[i].append(pltpu.make_async_remote_copy(
                src_ref=held.at[i], dst_ref=land.at[me, side],
                send_sem=send_sem.at[k, i], recv_sem=recv_sem.at[k, i],
                device_id={"span": targets[i]}, device_id_type=MESH,
            ))
            sent[i][-1].start()

    def hear(i):
        for k, (held, land) in enumerate(((stage, rows), (stage_rot, turned))):
            pltpu.make_async_remote_copy(
                src_ref=held.at[i], dst_ref=land.at[sources[i], side],
                send_sem=send_sem.at[k, i], recv_sem=recv_sem.at[k, i],
                device_id={"span": targets[i]}, device_id_type=MESH,
            ).wait_recv()
        passed.append(forward(sources[i], i + 1))

    def landed(q, i):
        for k, held in enumerate((rows, turned)):
            pltpu.make_async_remote_copy(
                src_ref=held.at[q, other], dst_ref=held.at[q, other],
                send_sem=pass_sem.at[k, i], recv_sem=land_sem.at[k, i],
                device_id={"heads": other}, device_id_type=MESH,
            ).wait_recv()

    def unravel(raw, size, put):
        piece = 128

        @pl.loop(0, depth // piece)
        def _(n):
            r = pl.multiple_of(n * piece, piece)
            part = raw[pl.ds(r, piece)].astype(jnp.float32)
            flat[pl.ds(0, piece * heads), :] = part.reshape(piece * heads, size)
            for h in range(heads):
                put(h, r, piece, flat[pl.ds(h, piece, stride=heads), :])

    def put_value(h, r, piece, block):
        value_wide[pl.ds(r, piece), h * value_width:(h + 1) * value_width] = block.astype(jnp.bfloat16)

    def put_key(h, r, piece, block):
        key_wide[h * width:(h + 1) * width, pl.ds(r, piece)] = block.T.astype(jnp.bfloat16)

    def expand(q):
        raw = rows[q].reshape(both, depth).astype(jnp.float32)
        ready = unit_rows(raw, gain[...]).astype(jnp.bfloat16)
        start = pl.multiple_of(q * both, both)
        for h in range(heads):
            wide = lax.dot_general(
                key_wide[h * width:(h + 1) * width, :], ready,
                (((1,), (1,)), ((), ())), preferred_element_type=jnp.float32,
            )
            keys[0, h, :width, pl.ds(start, both)] = wide.astype(jnp.bfloat16)
            for k in range(2):
                keys[0, h, width:width + turn, pl.ds(start + k * count, count)] = turned[q, k]
        pair = 2 * value_width
        for h in range(0, heads, 2):
            wide = jnp.dot(
                ready, value_wide[:, h * value_width:h * value_width + pair],
                preferred_element_type=jnp.float32,
            )
            for k in range(2):
                flat_out[pl.ds(h + k, both, stride=heads), :] = wide[:, k * value_width:(k + 1) * value_width]
        values[0, pl.ds(start, both)] = flat_out[...].reshape(both, heads, value_width).astype(jnp.bfloat16)

    hear(0)
    for copy in weights:
        copy.wait()
    unravel(raw_key, width, put_key)
    unravel(raw_value, value_width, put_value)
    for i in range(1, steps):
        hear(i)
        landed((me, *sources)[i - 1], i - 1)
        expand((me, *sources)[i - 1])
    for i in range(steps - 1, steps + 1):
        landed((me, *sources)[i], i)
        expand((me, *sources)[i])
    for pair in (*passed, *sent.values()):
        for copy in pair:
            copy.wait_send()


def shards(latents, rotary_rows, latent_gain, key_up, value_up):
    spans, sides = lax.axis_size("span"), lax.axis_size("heads")
    _, count, depth = latents.shape
    turn = rotary_rows.shape[2]
    heads, width, value_width = key_up.shape[1], key_up.shape[2], value_up.shape[2]
    if (
        latents.shape[0] != spans or spans % 2 or sides != 2 or count % 128 or depth % 128
        or heads % 8 or width != 128 or value_width != 128 or turn % 16
    ):
        return plain_shards(latents, rotary_rows, latent_gain, key_up, value_up)
    length = spans * sides * count
    far = pl.BlockSpec(memory_space=pltpu.HBM)
    steps = spans - 1
    bf16 = jnp.bfloat16
    keys, values = pl.pallas_call(
        functools.partial(exchange_kernel, spans),
        out_shape=(
            jax.ShapeDtypeStruct((1, heads, width + turn, length), bf16),
            jax.ShapeDtypeStruct((1, length, heads, value_width), bf16),
        ),
        in_specs=[far] * 5,
        out_specs=[pl.BlockSpec(memory_space=pltpu.VMEM)] * 2,
        scratch_shapes=[
            pltpu.VMEM((1, depth), jnp.float32),
            pltpu.VMEM((steps, count, depth), bf16),
            pltpu.VMEM((steps, turn, count), bf16),
            pltpu.VMEM((spans, sides, count, depth), bf16),
            pltpu.VMEM((spans, sides, turn, count), bf16),
            pltpu.VMEM(key_up.shape, bf16),
            pltpu.VMEM(value_up.shape, bf16),
            pltpu.VMEM((heads * width, depth), bf16),
            pltpu.VMEM((depth, heads * value_width), bf16),
            pltpu.VMEM((128 * heads, 128), jnp.float32),
            pltpu.VMEM((2 * count * heads, value_width), jnp.float32),
            pltpu.SemaphoreType.DMA((2, spans)),
            pltpu.SemaphoreType.DMA((3,)),
            pltpu.SemaphoreType.DMA((2, steps)),
            pltpu.SemaphoreType.DMA((2, steps)),
            pltpu.SemaphoreType.DMA((2, spans)),
            pltpu.SemaphoreType.DMA((2, spans)),
        ],
        compiler_params=pltpu.CompilerParams(
            collective_id=0, has_side_effects=True, vmem_limit_bytes=40 * 1024 * 1024
        ),
    )(latents, jnp.swapaxes(rotary_rows, 1, 2), latent_gain[None], key_up, value_up)
    return keys, values


def solution(mesh):
    return jax.shard_map(
        shards,
        mesh=mesh,
        in_specs=(
            P("trial", ("span", "heads"), None),
            P("trial", ("span", "heads"), None),
            P(),
            P("trial", "heads", None),
            P("trial", "heads", None),
        ),
        out_specs=(
            P(("trial", "span"), "heads", None, None),
            P(("trial", "span"), None, "heads", None),
        ),
        check_vma=False,
    )
```

```python
import functools

import jax
import jax.numpy as jnp
from jax import lax
from jax.experimental import pallas as pl
from jax.experimental.pallas import tpu as pltpu
from jax.sharding import PartitionSpec as P

MESH = pl.DeviceIdType.MESH


def widen_rows(rows, rotary, key_up, value_up):
    wide_keys = jnp.einsum(
        "btr,rhk->bthk", rows, key_up, preferred_element_type=jnp.float32
    ).astype(jnp.bfloat16)
    shared = jnp.broadcast_to(rotary[:, :, None], wide_keys.shape[:3] + rotary.shape[2:])
    wide_values = jnp.einsum(
        "btr,rhk->bthk", rows, value_up, preferred_element_type=jnp.float32
    ).astype(jnp.bfloat16)
    return (jnp.concatenate([wide_keys, shared], axis=-1), wide_values)


def unit_rows(vectors, row_gain):
    return (
        vectors * lax.rsqrt(jnp.mean(vectors * vectors, axis=-1, keepdims=True) + 1e-06) * row_gain
    )


def plain_shards(latents, rotary_rows, latent_gain, key_up, value_up):
    rows_ready = unit_rows(latents.astype(jnp.float32), latent_gain).astype(jnp.bfloat16)

    def move(block):
        block = lax.all_to_all(block, "span", split_axis=0, concat_axis=1, tiled=True)
        block = block.reshape(block.shape[0], lax.axis_size("span"), -1, block.shape[2])
        block = lax.all_gather(block, "heads", axis=2, tiled=True)
        return block.reshape(block.shape[0], -1, block.shape[3])

    cache_keys, cache_values = widen_rows(move(rows_ready), move(rotary_rows), key_up, value_up)
    return (jnp.transpose(cache_keys, (0, 2, 3, 1)), cache_values)


def sibling(p):
    return p + 1 - 2 * lax.rem(p, 2)


def unit(raw, gain):
    sides, count, depth = raw.shape
    raw = raw.reshape(sides * count, depth).astype(jnp.float32)
    return unit_rows(raw, gain[...]).astype(jnp.bfloat16)


def expand_keys(ready, turned, key_wide, keys):
    heads, turn, count = keys.shape[0], turned.shape[1], turned.shape[2]
    width = keys.shape[1] - turn
    for h in range(heads):
        wide = lax.dot_general(
            key_wide[h * width:(h + 1) * width, :], ready,
            (((1,), (1,)), ((), ())), preferred_element_type=jnp.float32,
        )
        keys[h, :width, :] = wide.astype(jnp.bfloat16)
        for k in range(turned.shape[0]):
            keys[h, width:width + turn, k * count:(k + 1) * count] = turned[k]


def expand_values(ready, value_wide, flat, values):
    both, heads, width = values.shape
    for h in range(0, heads, 2):
        wide = jnp.dot(
            ready, value_wide[:, h * width:(h + 2) * width], preferred_element_type=jnp.float32
        )
        for k in range(2):
            flat[pl.ds(h + k, both, stride=heads), :] = wide[:, k * width:(k + 1) * width]
    values[...] = flat[...].reshape(both, heads, width).astype(jnp.bfloat16)


def exchange_kernel(
    spans, lat, rot, far_gain, key_up, value_up, keys, values, rows_last, turned_last, key_wide, value_wide, gain,
    stage, stage_rot, rows, turned, raw_key, raw_value, flat, flat_out,
    load_sem, weight_sem, send_sem, recv_sem, pass_sem, land_sem,
):
    me, side = lax.axis_index("span"), lax.axis_index("heads")
    other = 1 - side
    count, depth = lat.shape[1], lat.shape[2]
    heads, width = key_up.shape[1], key_up.shape[2]
    value_width = value_up.shape[2]
    turn = rot.shape[1]
    both = 2 * count

    targets, sources = [sibling(me)], [sibling(me)]
    for j in range(1, spans // 2):
        ahead, behind = lax.rem(me + 2 * j, spans), lax.rem(me + spans - 2 * j, spans)
        targets += [ahead, sibling(ahead)]
        sources += [behind, lax.rem(sibling(me) + spans - 2 * j, spans)]
    steps = len(targets)

    barrier = pltpu.get_barrier_semaphore()
    for q in targets:
        pl.semaphore_signal(barrier, inc=1, device_id={"span": q}, device_id_type=MESH)
    pl.semaphore_signal(barrier, inc=1, device_id={"heads": other}, device_id_type=MESH)

    order = list(range(1, steps)) + [0]
    loads = {}
    own = (
        pltpu.make_async_copy(lat.at[me], rows.at[me, side], load_sem.at[0, steps]),
        pltpu.make_async_copy(rot.at[me], turned.at[me, side], load_sem.at[1, steps]),
    )
    for copy in own:
        copy.start()
    for i in order:
        loads[i] = (
            pltpu.make_async_copy(lat.at[targets[i]], stage.at[i], load_sem.at[0, i]),
            pltpu.make_async_copy(rot.at[targets[i]], stage_rot.at[i], load_sem.at[1, i]),
        )
        for copy in loads[i]:
            copy.start()
    weights = (
        pltpu.make_async_copy(key_up, raw_key, weight_sem.at[0]),
        pltpu.make_async_copy(value_up, raw_value, weight_sem.at[1]),
        pltpu.make_async_copy(far_gain, gain, weight_sem.at[2]),
    )
    for copy in weights:
        copy.start()
    pl.semaphore_wait(barrier, steps + 1)

    def forward(q, i):
        made = []
        for k, held in enumerate((rows, turned)):
            made.append(pltpu.make_async_remote_copy(
                src_ref=held.at[q, side], dst_ref=held.at[q, side],
                send_sem=pass_sem.at[k, i], recv_sem=land_sem.at[k, i],
                device_id={"heads": other}, device_id_type=MESH,
            ))
            made[-1].start()
        return made

    for copy in own:
        copy.wait()
    passed = [forward(me, 0)]
    sent = {}
    for i in order:
        for copy in loads[i]:
            copy.wait()
        sent[i] = []
        for k, (held, land) in enumerate(((stage, rows), (stage_rot, turned))):
            sent[i].append(pltpu.make_async_remote_copy(
                src_ref=held.at[i], dst_ref=land.at[me, side],
                send_sem=send_sem.at[k, i], recv_sem=recv_sem.at[k, i],
                device_id={"span": targets[i]}, device_id_type=MESH,
            ))
            sent[i][-1].start()

    def hear(i):
        for k, (held, land) in enumerate(((stage, rows), (stage_rot, turned))):
            pltpu.make_async_remote_copy(
                src_ref=held.at[i], dst_ref=land.at[sources[i], side],
                send_sem=send_sem.at[k, i], recv_sem=recv_sem.at[k, i],
                device_id={"span": targets[i]}, device_id_type=MESH,
            ).wait_recv()
        passed.append(forward(sources[i], i + 1))

    def landed(q, i):
        for k, held in enumerate((rows, turned)):
            pltpu.make_async_remote_copy(
                src_ref=held.at[q, other], dst_ref=held.at[q, other],
                send_sem=pass_sem.at[k, i], recv_sem=land_sem.at[k, i],
                device_id={"heads": other}, device_id_type=MESH,
            ).wait_recv()

    def unravel(raw, size, put):
        piece = 128

        @pl.loop(0, depth // piece)
        def _(n):
            r = pl.multiple_of(n * piece, piece)
            part = raw[pl.ds(r, piece)].astype(jnp.float32)
            flat[pl.ds(0, piece * heads), :] = part.reshape(piece * heads, size)
            for h in range(heads):
                put(h, r, piece, flat[pl.ds(h, piece, stride=heads), :])

    def put_value(h, r, piece, block):
        value_wide[pl.ds(r, piece), h * value_width:(h + 1) * value_width] = block.astype(jnp.bfloat16)

    def put_key(h, r, piece, block):
        key_wide[h * width:(h + 1) * width, pl.ds(r, piece)] = block.T.astype(jnp.bfloat16)

    hear(0)
    for copy in weights:
        copy.wait()
    unravel(raw_key, width, put_key)
    unravel(raw_value, value_width, put_value)
    def finish(q):
        start = pl.multiple_of(q * both, both)
        expand_keys(
            unit(rows[q], gain), turned.at[q], key_wide, keys.at[:, :, pl.ds(start, both)]
        )
        expand_values(
            unit(rows[q], gain), value_wide, flat_out, values.at[pl.ds(start, both)]
        )

    for i in range(1, steps):
        hear(i)
        landed((me, *sources)[i - 1], i - 1)
        finish((me, *sources)[i - 1])
    landed(sources[steps - 2], steps - 1)
    finish(sources[steps - 2])
    last = sources[steps - 1]
    landed(last, steps)
    rows_last[...] = rows[last]
    turned_last[...] = turned[last]
    for pair in (*passed, *sent.values()):
        for copy in pair:
            copy.wait_send()


def write_kernel(
    spans, keys_part, values_part, rows_last, turned_last, key_wide, value_wide, gain,
    keys, values, keys_last, values_last, flat, sem, last_sem,
):
    me = lax.axis_index("span")
    both = values_last.shape[0]
    order = [me, sibling(me)]
    for j in range(1, spans // 2):
        behind = lax.rem(me + spans - 2 * j, spans)
        order += [behind, lax.rem(sibling(me) + spans - 2 * j, spans)]
    copies = []
    for i, q in enumerate(order[:-1]):
        at = pl.ds(pl.multiple_of(q * both, both), both)
        copies += [
            pltpu.make_async_copy(keys_part.at[:, :, at], keys.at[0, :, :, at], sem.at[0, i]),
            pltpu.make_async_copy(values_part.at[at], values.at[0, at], sem.at[1, i]),
        ]
    for copy in copies:
        copy.start()
    at = pl.ds(pl.multiple_of(order[-1] * both, both), both)
    ready = unit(rows_last[...], gain)
    expand_keys(ready, turned_last, key_wide, keys_last)
    copies.append(pltpu.make_async_copy(keys_last, keys.at[0, :, :, at], last_sem.at[0]))
    copies[-1].start()
    expand_values(ready, value_wide, flat, values_last)
    copies.append(pltpu.make_async_copy(values_last, values.at[0, at], last_sem.at[1]))
    copies[-1].start()
    for copy in copies:
        copy.wait()


def shards(latents, rotary_rows, latent_gain, key_up, value_up):
    spans, sides = lax.axis_size("span"), lax.axis_size("heads")
    _, count, depth = latents.shape
    turn = rotary_rows.shape[2]
    heads, width, value_width = key_up.shape[1], key_up.shape[2], value_up.shape[2]
    if (
        latents.shape[0] != spans or spans % 2 or sides != 2 or count % 128 or depth % 128
        or heads % 8 or width != 128 or value_width != 128 or turn % 16
    ):
        return plain_shards(latents, rotary_rows, latent_gain, key_up, value_up)
    length, both = spans * sides * count, sides * count
    steps = spans - 1
    bf16, f32 = jnp.bfloat16, jnp.float32
    near = pl.BlockSpec(memory_space=pltpu.VMEM)
    far = pl.BlockSpec(memory_space=pltpu.HBM)
    args = (latents, jnp.swapaxes(rotary_rows, 1, 2), latent_gain[None], key_up, value_up)
    parts = pl.pallas_call(
        functools.partial(exchange_kernel, spans),
        out_shape=(
            pltpu.VMEM((heads, width + turn, length), bf16),
            pltpu.VMEM((length, heads, value_width), bf16),
            pltpu.VMEM((sides, count, depth), bf16),
            pltpu.VMEM((sides, turn, count), bf16),
            pltpu.VMEM((heads * width, depth), bf16),
            pltpu.VMEM((depth, heads * value_width), bf16),
            pltpu.VMEM((1, depth), f32),
        ),
        in_specs=[far] * 5,
        out_specs=[near] * 7,
        scratch_shapes=[
            pltpu.VMEM((steps, count, depth), bf16),
            pltpu.VMEM((steps, turn, count), bf16),
            pltpu.VMEM((spans, sides, count, depth), bf16),
            pltpu.VMEM((spans, sides, turn, count), bf16),
            pltpu.VMEM(key_up.shape, bf16),
            pltpu.VMEM(value_up.shape, bf16),
            pltpu.VMEM((128 * heads, 128), f32),
            pltpu.VMEM((both * heads, value_width), f32),
            pltpu.SemaphoreType.DMA((2, spans)),
            pltpu.SemaphoreType.DMA((3,)),
            pltpu.SemaphoreType.DMA((2, steps)),
            pltpu.SemaphoreType.DMA((2, steps)),
            pltpu.SemaphoreType.DMA((2, spans)),
            pltpu.SemaphoreType.DMA((2, spans)),
        ],
        compiler_params=pltpu.CompilerParams(
            collective_id=0, has_side_effects=True, vmem_limit_bytes=40 * 1024 * 1024
        ),
    )(*(pltpu.with_memory_space_constraint(arg, pltpu.HBM) for arg in args))
    return pl.pallas_call(
        functools.partial(write_kernel, spans),
        out_shape=(
            jax.ShapeDtypeStruct((1, heads, width + turn, length), bf16),
            jax.ShapeDtypeStruct((1, length, heads, value_width), bf16),
        ),
        in_specs=[near] * 7,
        out_specs=[far] * 2,
        scratch_shapes=[
            pltpu.VMEM((heads, width + turn, both), bf16),
            pltpu.VMEM((both, heads, value_width), bf16),
            pltpu.VMEM((both * heads, value_width), f32),
            pltpu.SemaphoreType.DMA((2, steps)),
            pltpu.SemaphoreType.DMA((2,)),
        ],
        compiler_params=pltpu.CompilerParams(vmem_limit_bytes=16 * 1024 * 1024),
    )(*parts)


def solution(mesh):
    return jax.shard_map(
        shards,
        mesh=mesh,
        in_specs=(
            P("trial", ("span", "heads"), None),
            P("trial", ("span", "heads"), None),
            P(),
            P("trial", "heads", None),
            P("trial", "heads", None),
        ),
        out_specs=(
            P(("trial", "span"), "heads", None, None),
            P(("trial", "span"), None, "heads", None),
        ),
        check_vma=False,
    )
```

```python
import functools

import jax
import jax.numpy as jnp
from jax import lax
from jax.experimental import pallas as pl
from jax.experimental.pallas import tpu as pltpu
from jax.sharding import PartitionSpec as P

MESH = pl.DeviceIdType.MESH


def widen_rows(rows, rotary, key_up, value_up):
    wide_keys = jnp.einsum(
        "btr,rhk->bthk", rows, key_up, preferred_element_type=jnp.float32
    ).astype(jnp.bfloat16)
    shared = jnp.broadcast_to(rotary[:, :, None], wide_keys.shape[:3] + rotary.shape[2:])
    wide_values = jnp.einsum(
        "btr,rhk->bthk", rows, value_up, preferred_element_type=jnp.float32
    ).astype(jnp.bfloat16)
    return (jnp.concatenate([wide_keys, shared], axis=-1), wide_values)


def unit_rows(vectors, row_gain):
    return (
        vectors * lax.rsqrt(jnp.mean(vectors * vectors, axis=-1, keepdims=True) + 1e-06) * row_gain
    )


def plain_shards(latents, rotary_rows, latent_gain, key_up, value_up):
    rows_ready = unit_rows(latents.astype(jnp.float32), latent_gain).astype(jnp.bfloat16)

    def move(block):
        block = lax.all_to_all(block, "span", split_axis=0, concat_axis=1, tiled=True)
        block = block.reshape(block.shape[0], lax.axis_size("span"), -1, block.shape[2])
        block = lax.all_gather(block, "heads", axis=2, tiled=True)
        return block.reshape(block.shape[0], -1, block.shape[3])

    cache_keys, cache_values = widen_rows(move(rows_ready), move(rotary_rows), key_up, value_up)
    return (jnp.transpose(cache_keys, (0, 2, 3, 1)), cache_values)


def sibling(p):
    return p + 1 - 2 * lax.rem(p, 2)


def unit(raw, gain):
    sides, count, depth = raw.shape
    raw = raw.reshape(sides * count, depth).astype(jnp.float32)
    return unit_rows(raw, gain[...]).astype(jnp.bfloat16)


def expand_keys(ready, turned, key_wide, keys):
    heads, turn, count = keys.shape[0], turned.shape[1], turned.shape[2]
    width = keys.shape[1] - turn
    for h in range(heads):
        wide = lax.dot_general(
            key_wide[h * width:(h + 1) * width, :], ready,
            (((1,), (1,)), ((), ())), preferred_element_type=jnp.float32,
        )
        keys[h, :width, :] = wide.astype(jnp.bfloat16)
        for k in range(turned.shape[0]):
            keys[h, width:width + turn, k * count:(k + 1) * count] = turned[k]


def expand_values(ready, value_wide, flat, values):
    both, heads, width = values.shape
    for h in range(0, heads, 2):
        wide = jnp.dot(
            ready, value_wide[:, h * width:(h + 2) * width], preferred_element_type=jnp.float32
        )
        for k in range(2):
            flat[pl.ds(h + k, both, stride=heads), :] = wide[:, k * width:(k + 1) * width]
    values[...] = flat[pl.ds(0, both * heads), :].reshape(both, heads, width).astype(jnp.bfloat16)


def exchange_kernel(
    spans, lat, rot, far_gain, key_up, value_up, keys, values, rows_last, turned_last, key_wide, value_wide, gain,
    stage, stage_rot, rows, turned, raw_key, raw_value, flat, flat_out,
    load_sem, weight_sem, send_sem, recv_sem, pass_sem, land_sem,
):
    me, side = lax.axis_index("span"), lax.axis_index("heads")
    other = 1 - side
    count, depth = lat.shape[1], lat.shape[2]
    heads, width = key_up.shape[1], key_up.shape[2]
    value_width = value_up.shape[2]
    turn = rot.shape[1]
    both = 2 * count

    targets, sources = [sibling(me)], [sibling(me)]
    for j in range(1, spans // 2):
        ahead, behind = lax.rem(me + 2 * j, spans), lax.rem(me + spans - 2 * j, spans)
        targets += [ahead, sibling(ahead)]
        sources += [behind, lax.rem(sibling(me) + spans - 2 * j, spans)]
    steps = len(targets)

    barrier = pltpu.get_barrier_semaphore()
    for q in targets:
        pl.semaphore_signal(barrier, inc=1, device_id={"span": q}, device_id_type=MESH)
    pl.semaphore_signal(barrier, inc=1, device_id={"heads": other}, device_id_type=MESH)

    order = list(range(1, steps)) + [0]
    loads = {}
    own = (
        pltpu.make_async_copy(lat.at[me], rows.at[me, side], load_sem.at[0, steps]),
        pltpu.make_async_copy(rot.at[me], turned.at[me, side], load_sem.at[1, steps]),
    )
    for copy in own:
        copy.start()
    for i in order:
        loads[i] = (
            pltpu.make_async_copy(lat.at[targets[i]], stage.at[i], load_sem.at[0, i]),
            pltpu.make_async_copy(rot.at[targets[i]], stage_rot.at[i], load_sem.at[1, i]),
        )
        for copy in loads[i]:
            copy.start()
    weights = (
        pltpu.make_async_copy(key_up, raw_key, weight_sem.at[0]),
        pltpu.make_async_copy(value_up, raw_value, weight_sem.at[1]),
        pltpu.make_async_copy(far_gain, gain, weight_sem.at[2]),
    )
    for copy in weights:
        copy.start()
    pl.semaphore_wait(barrier, steps + 1)

    def forward(q, i):
        made = []
        for k, held in enumerate((rows, turned)):
            made.append(pltpu.make_async_remote_copy(
                src_ref=held.at[q, side], dst_ref=held.at[q, side],
                send_sem=pass_sem.at[k, i], recv_sem=land_sem.at[k, i],
                device_id={"heads": other}, device_id_type=MESH,
            ))
            made[-1].start()
        return made

    for copy in own:
        copy.wait()
    passed = [forward(me, 0)]
    sent = {}
    for i in order:
        for copy in loads[i]:
            copy.wait()
        sent[i] = []
        for k, (held, land) in enumerate(((stage, rows), (stage_rot, turned))):
            sent[i].append(pltpu.make_async_remote_copy(
                src_ref=held.at[i], dst_ref=land.at[me, side],
                send_sem=send_sem.at[k, i], recv_sem=recv_sem.at[k, i],
                device_id={"span": targets[i]}, device_id_type=MESH,
            ))
            sent[i][-1].start()

    def hear(i):
        for k, (held, land) in enumerate(((stage, rows), (stage_rot, turned))):
            pltpu.make_async_remote_copy(
                src_ref=held.at[i], dst_ref=land.at[sources[i], side],
                send_sem=send_sem.at[k, i], recv_sem=recv_sem.at[k, i],
                device_id={"span": targets[i]}, device_id_type=MESH,
            ).wait_recv()
        passed.append(forward(sources[i], i + 1))

    def landed(q, i):
        for k, held in enumerate((rows, turned)):
            pltpu.make_async_remote_copy(
                src_ref=held.at[q, other], dst_ref=held.at[q, other],
                send_sem=pass_sem.at[k, i], recv_sem=land_sem.at[k, i],
                device_id={"heads": other}, device_id_type=MESH,
            ).wait_recv()

    def unravel(raw, size, put):
        piece = 128

        @pl.loop(0, depth // piece)
        def _(n):
            r = pl.multiple_of(n * piece, piece)
            part = raw[pl.ds(r, piece)].astype(jnp.float32)
            flat[pl.ds(0, piece * heads), :] = part.reshape(piece * heads, size)
            for h in range(heads):
                put(h, r, piece, flat[pl.ds(h, piece, stride=heads), :])

    def put_value(h, r, piece, block):
        value_wide[pl.ds(r, piece), h * value_width:(h + 1) * value_width] = block.astype(jnp.bfloat16)

    def put_key(h, r, piece, block):
        key_wide[h * width:(h + 1) * width, pl.ds(r, piece)] = block.T.astype(jnp.bfloat16)

    hear(0)
    for copy in weights:
        copy.wait()
    unravel(raw_key, width, put_key)
    unravel(raw_value, value_width, put_value)
    def finish(q):
        start = pl.multiple_of(q * both, both)
        expand_keys(
            unit(rows[q], gain), turned.at[q], key_wide, keys.at[:, :, pl.ds(start, both)]
        )
        expand_values(
            unit(rows[q], gain), value_wide, flat_out, values.at[pl.ds(start, both)]
        )

    for i in range(1, steps):
        hear(i)
        landed((me, *sources)[i - 1], i - 1)
        finish((me, *sources)[i - 1])
    last = sources[steps - 1]
    start = pl.multiple_of(last * both + side * count, count)
    half = pl.ds(side, 1)
    expand_keys(
        unit(rows[last, half], gain), turned.at[last, half], key_wide,
        keys.at[:, :, pl.ds(start, count)],
    )
    expand_values(
        unit(rows[last, half], gain), value_wide, flat_out, values.at[pl.ds(start, count)]
    )
    landed(sources[steps - 2], steps - 1)
    finish(sources[steps - 2])
    landed(last, steps)
    rows_last[...] = rows[last, pl.ds(other, 1)]
    turned_last[...] = turned[last, pl.ds(other, 1)]
    for pair in (*passed, *sent.values()):
        for copy in pair:
            copy.wait_send()


def write_kernel(
    spans, keys_part, values_part, rows_last, turned_last, key_wide, value_wide, gain,
    keys, values, keys_last, values_last, flat, sem, last_sem,
):
    me, side = lax.axis_index("span"), lax.axis_index("heads")
    count = values_last.shape[0]
    both = 2 * count
    order = [me, sibling(me)]
    for j in range(1, spans // 2):
        behind = lax.rem(me + spans - 2 * j, spans)
        order += [behind, lax.rem(sibling(me) + spans - 2 * j, spans)]
    last = order[-1] * both
    done = [pl.ds(pl.multiple_of(q * both, both), both) for q in order[:-1]]
    done.append(pl.ds(pl.multiple_of(last + side * count, count), count))
    copies = []
    for i, at in enumerate(done):
        copies += [
            pltpu.make_async_copy(keys_part.at[:, :, at], keys.at[0, :, :, at], sem.at[0, i]),
            pltpu.make_async_copy(values_part.at[at], values.at[0, at], sem.at[1, i]),
        ]
    for copy in copies:
        copy.start()
    at = pl.ds(pl.multiple_of(last + (1 - side) * count, count), count)
    ready = unit(rows_last[...], gain)
    expand_keys(ready, turned_last, key_wide, keys_last)
    copies.append(pltpu.make_async_copy(keys_last, keys.at[0, :, :, at], last_sem.at[0]))
    copies[-1].start()
    expand_values(ready, value_wide, flat, values_last)
    copies.append(pltpu.make_async_copy(values_last, values.at[0, at], last_sem.at[1]))
    copies[-1].start()
    for copy in copies:
        copy.wait()


def shards(latents, rotary_rows, latent_gain, key_up, value_up):
    spans, sides = lax.axis_size("span"), lax.axis_size("heads")
    _, count, depth = latents.shape
    turn = rotary_rows.shape[2]
    heads, width, value_width = key_up.shape[1], key_up.shape[2], value_up.shape[2]
    if (
        latents.shape[0] != spans or spans % 2 or sides != 2 or count % 128 or depth % 128
        or heads % 8 or width != 128 or value_width != 128 or turn % 16
    ):
        return plain_shards(latents, rotary_rows, latent_gain, key_up, value_up)
    length, both = spans * sides * count, sides * count
    steps = spans - 1
    bf16, f32 = jnp.bfloat16, jnp.float32
    near = pl.BlockSpec(memory_space=pltpu.VMEM)
    far = pl.BlockSpec(memory_space=pltpu.HBM)
    args = (latents, jnp.swapaxes(rotary_rows, 1, 2), latent_gain[None], key_up, value_up)
    parts = pl.pallas_call(
        functools.partial(exchange_kernel, spans),
        out_shape=(
            pltpu.VMEM((heads, width + turn, length), bf16),
            pltpu.VMEM((length, heads, value_width), bf16),
            pltpu.VMEM((1, count, depth), bf16),
            pltpu.VMEM((1, turn, count), bf16),
            pltpu.VMEM((heads * width, depth), bf16),
            pltpu.VMEM((depth, heads * value_width), bf16),
            pltpu.VMEM((1, depth), f32),
        ),
        in_specs=[far] * 5,
        out_specs=[near] * 7,
        scratch_shapes=[
            pltpu.VMEM((steps, count, depth), bf16),
            pltpu.VMEM((steps, turn, count), bf16),
            pltpu.VMEM((spans, sides, count, depth), bf16),
            pltpu.VMEM((spans, sides, turn, count), bf16),
            pltpu.VMEM(key_up.shape, bf16),
            pltpu.VMEM(value_up.shape, bf16),
            pltpu.VMEM((128 * heads, 128), f32),
            pltpu.VMEM((both * heads, value_width), f32),
            pltpu.SemaphoreType.DMA((2, spans)),
            pltpu.SemaphoreType.DMA((3,)),
            pltpu.SemaphoreType.DMA((2, steps)),
            pltpu.SemaphoreType.DMA((2, steps)),
            pltpu.SemaphoreType.DMA((2, spans)),
            pltpu.SemaphoreType.DMA((2, spans)),
        ],
        compiler_params=pltpu.CompilerParams(
            collective_id=0, has_side_effects=True, vmem_limit_bytes=40 * 1024 * 1024
        ),
    )(*(pltpu.with_memory_space_constraint(arg, pltpu.HBM) for arg in args))
    return pl.pallas_call(
        functools.partial(write_kernel, spans),
        out_shape=(
            jax.ShapeDtypeStruct((1, heads, width + turn, length), bf16),
            jax.ShapeDtypeStruct((1, length, heads, value_width), bf16),
        ),
        in_specs=[near] * 7,
        out_specs=[far] * 2,
        scratch_shapes=[
            pltpu.VMEM((heads, width + turn, count), bf16),
            pltpu.VMEM((count, heads, value_width), bf16),
            pltpu.VMEM((count * heads, value_width), f32),
            pltpu.SemaphoreType.DMA((2, spans)),
            pltpu.SemaphoreType.DMA((2,)),
        ],
        compiler_params=pltpu.CompilerParams(vmem_limit_bytes=16 * 1024 * 1024),
    )(*parts)


def solution(mesh):
    return jax.shard_map(
        shards,
        mesh=mesh,
        in_specs=(
            P("trial", ("span", "heads"), None),
            P("trial", ("span", "heads"), None),
            P(),
            P("trial", "heads", None),
            P("trial", "heads", None),
        ),
        out_specs=(
            P(("trial", "span"), "heads", None, None),
            P(("trial", "span"), None, "heads", None),
        ),
        check_vma=False,
    )
```

```python
import functools

import jax
import jax.numpy as jnp
from jax import lax
from jax.experimental import pallas as pl
from jax.experimental.pallas import tpu as pltpu
from jax.sharding import PartitionSpec as P

MESH = pl.DeviceIdType.MESH


def widen_rows(rows, rotary, key_up, value_up):
    wide_keys = jnp.einsum(
        "btr,rhk->bthk", rows, key_up, preferred_element_type=jnp.float32
    ).astype(jnp.bfloat16)
    shared = jnp.broadcast_to(rotary[:, :, None], wide_keys.shape[:3] + rotary.shape[2:])
    wide_values = jnp.einsum(
        "btr,rhk->bthk", rows, value_up, preferred_element_type=jnp.float32
    ).astype(jnp.bfloat16)
    return (jnp.concatenate([wide_keys, shared], axis=-1), wide_values)


def unit_rows(vectors, row_gain):
    return (
        vectors * lax.rsqrt(jnp.mean(vectors * vectors, axis=-1, keepdims=True) + 1e-06) * row_gain
    )


def plain_shards(latents, rotary_rows, latent_gain, key_up, value_up):
    rows_ready = unit_rows(latents.astype(jnp.float32), latent_gain).astype(jnp.bfloat16)

    def move(block):
        block = lax.all_to_all(block, "span", split_axis=0, concat_axis=1, tiled=True)
        block = block.reshape(block.shape[0], lax.axis_size("span"), -1, block.shape[2])
        block = lax.all_gather(block, "heads", axis=2, tiled=True)
        return block.reshape(block.shape[0], -1, block.shape[3])

    cache_keys, cache_values = widen_rows(move(rows_ready), move(rotary_rows), key_up, value_up)
    return (jnp.transpose(cache_keys, (0, 2, 3, 1)), cache_values)


def sibling(p):
    return p + 1 - 2 * lax.rem(p, 2)


def unit(raw, gain):
    sides, count, depth = raw.shape
    raw = raw.reshape(sides * count, depth).astype(jnp.float32)
    return unit_rows(raw, gain[...]).astype(jnp.bfloat16)


def expand_keys(ready, turned, key_wide, keys):
    heads, turn, count = keys.shape[0], turned.shape[1], turned.shape[2]
    width = keys.shape[1] - turn
    for h in range(heads):
        wide = lax.dot_general(
            key_wide[h * width:(h + 1) * width, :], ready,
            (((1,), (1,)), ((), ())), preferred_element_type=jnp.float32,
        )
        keys[h, :width, :] = wide.astype(jnp.bfloat16)
        for k in range(turned.shape[0]):
            keys[h, width:width + turn, k * count:(k + 1) * count] = turned[k]


def expand_values(ready, value_wide, flat, values):
    both, heads, width = values.shape
    for h in range(0, heads, 2):
        wide = jnp.dot(
            ready, value_wide[:, h * width:(h + 2) * width], preferred_element_type=jnp.float32
        )
        for k in range(2):
            flat[pl.ds(h + k, both, stride=heads), :] = wide[:, k * width:(k + 1) * width]
    values[...] = flat[pl.ds(0, both * heads), :].reshape(both, heads, width).astype(jnp.bfloat16)


def exchange_kernel(
    spans, lat, rot, far_gain, key_up, value_up, keys, values, rows_last, turned_last, key_wide, value_wide, gain,
    stage, stage_rot, rows, turned, raw_key, raw_value, flat, flat_out,
    load_sem, weight_sem, send_sem, recv_sem, pass_sem, land_sem, go_sem,
):
    me, side = lax.axis_index("span"), lax.axis_index("heads")
    other = 1 - side
    count, depth = lat.shape[1], lat.shape[2]
    heads, width = key_up.shape[1], key_up.shape[2]
    value_width = value_up.shape[2]
    turn = rot.shape[1]
    both = 2 * count

    targets, sources = [sibling(me)], [sibling(me)]
    for j in range(1, spans // 2):
        ahead, behind = lax.rem(me + 2 * j, spans), lax.rem(me + spans - 2 * j, spans)
        targets += [ahead, sibling(ahead)]
        sources += [behind, lax.rem(sibling(me) + spans - 2 * j, spans)]
    steps = len(targets)

    barrier = pltpu.get_barrier_semaphore()
    leader = spans - 1
    pl.semaphore_signal(barrier, inc=1, device_id={"heads": other}, device_id_type=MESH)

    @pl.when(me != leader)
    def _():
        pl.semaphore_signal(barrier, inc=1, device_id={"span": leader}, device_id_type=MESH)

    order = list(range(1, steps)) + [0]
    loads = {}
    own = (
        pltpu.make_async_copy(lat.at[me], rows.at[me, side], load_sem.at[0, steps]),
        pltpu.make_async_copy(rot.at[me], turned.at[me, side], load_sem.at[1, steps]),
    )
    for copy in own:
        copy.start()
    for i in order:
        loads[i] = (
            pltpu.make_async_copy(lat.at[targets[i]], stage.at[i], load_sem.at[0, i]),
            pltpu.make_async_copy(rot.at[targets[i]], stage_rot.at[i], load_sem.at[1, i]),
        )
        for copy in loads[i]:
            copy.start()
    weights = (
        pltpu.make_async_copy(key_up, raw_key, weight_sem.at[0]),
        pltpu.make_async_copy(value_up, raw_value, weight_sem.at[1]),
        pltpu.make_async_copy(far_gain, gain, weight_sem.at[2]),
    )
    for copy in weights:
        copy.start()

    @pl.when(me == leader)
    def _():
        pl.semaphore_wait(barrier, spans)
        for q in range(spans - 1):
            pl.semaphore_signal(go_sem, inc=1, device_id={"span": q}, device_id_type=MESH)

    @pl.when(me != leader)
    def _():
        pl.semaphore_wait(barrier, 1)

    def forward(q, i):
        made = []
        for k, held in enumerate((rows, turned)):
            made.append(pltpu.make_async_remote_copy(
                src_ref=held.at[q, side], dst_ref=held.at[q, side],
                send_sem=pass_sem.at[k, i], recv_sem=land_sem.at[k, i],
                device_id={"heads": other}, device_id_type=MESH,
            ))
            made[-1].start()
        return made

    for copy in own:
        copy.wait()
    passed = [forward(me, 0)]

    @pl.when(me != leader)
    def _():
        pl.semaphore_wait(go_sem, 1)

    sent = {}
    for i in order:
        for copy in loads[i]:
            copy.wait()
        sent[i] = []
        for k, (held, land) in enumerate(((stage, rows), (stage_rot, turned))):
            sent[i].append(pltpu.make_async_remote_copy(
                src_ref=held.at[i], dst_ref=land.at[me, side],
                send_sem=send_sem.at[k, i], recv_sem=recv_sem.at[k, i],
                device_id={"span": targets[i]}, device_id_type=MESH,
            ))
            sent[i][-1].start()

    def hear(i):
        for k, (held, land) in enumerate(((stage, rows), (stage_rot, turned))):
            pltpu.make_async_remote_copy(
                src_ref=held.at[i], dst_ref=land.at[sources[i], side],
                send_sem=send_sem.at[k, i], recv_sem=recv_sem.at[k, i],
                device_id={"span": targets[i]}, device_id_type=MESH,
            ).wait_recv()
        passed.append(forward(sources[i], i + 1))

    def landed(q, i):
        for k, held in enumerate((rows, turned)):
            pltpu.make_async_remote_copy(
                src_ref=held.at[q, other], dst_ref=held.at[q, other],
                send_sem=pass_sem.at[k, i], recv_sem=land_sem.at[k, i],
                device_id={"heads": other}, device_id_type=MESH,
            ).wait_recv()

    def unravel(raw, size, put):
        piece = 128

        @pl.loop(0, depth // piece)
        def _(n):
            r = pl.multiple_of(n * piece, piece)
            part = raw[pl.ds(r, piece)].astype(jnp.float32)
            flat[pl.ds(0, piece * heads), :] = part.reshape(piece * heads, size)
            for h in range(heads):
                put(h, r, piece, flat[pl.ds(h, piece, stride=heads), :])

    def put_value(h, r, piece, block):
        value_wide[pl.ds(r, piece), h * value_width:(h + 1) * value_width] = block.astype(jnp.bfloat16)

    def put_key(h, r, piece, block):
        key_wide[h * width:(h + 1) * width, pl.ds(r, piece)] = block.T.astype(jnp.bfloat16)

    hear(0)
    for copy in weights:
        copy.wait()
    unravel(raw_key, width, put_key)
    unravel(raw_value, value_width, put_value)
    def finish(q):
        start = pl.multiple_of(q * both, both)
        expand_keys(
            unit(rows[q], gain), turned.at[q], key_wide, keys.at[:, :, pl.ds(start, both)]
        )
        expand_values(
            unit(rows[q], gain), value_wide, flat_out, values.at[pl.ds(start, both)]
        )

    for i in range(1, steps):
        hear(i)
        landed((me, *sources)[i - 1], i - 1)
        finish((me, *sources)[i - 1])
    last = sources[steps - 1]
    start = pl.multiple_of(last * both + side * count, count)
    half = pl.ds(side, 1)
    expand_keys(
        unit(rows[last, half], gain), turned.at[last, half], key_wide,
        keys.at[:, :, pl.ds(start, count)],
    )
    expand_values(
        unit(rows[last, half], gain), value_wide, flat_out, values.at[pl.ds(start, count)]
    )
    landed(sources[steps - 2], steps - 1)
    finish(sources[steps - 2])
    landed(last, steps)
    rows_last[...] = rows[last, pl.ds(other, 1)]
    turned_last[...] = turned[last, pl.ds(other, 1)]
    for pair in (*passed, *sent.values()):
        for copy in pair:
            copy.wait_send()


def write_kernel(
    spans, keys_part, values_part, rows_last, turned_last, key_wide, value_wide, gain,
    keys, values, keys_last, values_last, flat, sem, last_sem,
):
    me, side = lax.axis_index("span"), lax.axis_index("heads")
    count = values_last.shape[0]
    both = 2 * count
    order = [me, sibling(me)]
    for j in range(1, spans // 2):
        behind = lax.rem(me + spans - 2 * j, spans)
        order += [behind, lax.rem(sibling(me) + spans - 2 * j, spans)]
    last = order[-1] * both
    done = [pl.ds(pl.multiple_of(q * both, both), both) for q in order[:-1]]
    done.append(pl.ds(pl.multiple_of(last + side * count, count), count))
    copies = []
    for i, at in enumerate(done):
        copies += [
            pltpu.make_async_copy(keys_part.at[:, :, at], keys.at[0, :, :, at], sem.at[0, i]),
            pltpu.make_async_copy(values_part.at[at], values.at[0, at], sem.at[1, i]),
        ]
    for copy in copies:
        copy.start()
    at = pl.ds(pl.multiple_of(last + (1 - side) * count, count), count)
    ready = unit(rows_last[...], gain)
    expand_keys(ready, turned_last, key_wide, keys_last)
    copies.append(pltpu.make_async_copy(keys_last, keys.at[0, :, :, at], last_sem.at[0]))
    copies[-1].start()
    expand_values(ready, value_wide, flat, values_last)
    copies.append(pltpu.make_async_copy(values_last, values.at[0, at], last_sem.at[1]))
    copies[-1].start()
    for copy in copies:
        copy.wait()


def shards(latents, rotary_rows, latent_gain, key_up, value_up):
    spans, sides = lax.axis_size("span"), lax.axis_size("heads")
    _, count, depth = latents.shape
    turn = rotary_rows.shape[2]
    heads, width, value_width = key_up.shape[1], key_up.shape[2], value_up.shape[2]
    if (
        latents.shape[0] != spans or spans % 2 or sides != 2 or count % 128 or depth % 128
        or heads % 8 or width != 128 or value_width != 128 or turn % 16
    ):
        return plain_shards(latents, rotary_rows, latent_gain, key_up, value_up)
    length, both = spans * sides * count, sides * count
    steps = spans - 1
    bf16, f32 = jnp.bfloat16, jnp.float32
    near = pl.BlockSpec(memory_space=pltpu.VMEM)
    far = pl.BlockSpec(memory_space=pltpu.HBM)
    args = (latents, jnp.swapaxes(rotary_rows, 1, 2), latent_gain[None], key_up, value_up)
    parts = pl.pallas_call(
        functools.partial(exchange_kernel, spans),
        out_shape=(
            pltpu.VMEM((heads, width + turn, length), bf16),
            pltpu.VMEM((length, heads, value_width), bf16),
            pltpu.VMEM((1, count, depth), bf16),
            pltpu.VMEM((1, turn, count), bf16),
            pltpu.VMEM((heads * width, depth), bf16),
            pltpu.VMEM((depth, heads * value_width), bf16),
            pltpu.VMEM((1, depth), f32),
        ),
        in_specs=[far] * 5,
        out_specs=[near] * 7,
        scratch_shapes=[
            pltpu.VMEM((steps, count, depth), bf16),
            pltpu.VMEM((steps, turn, count), bf16),
            pltpu.VMEM((spans, sides, count, depth), bf16),
            pltpu.VMEM((spans, sides, turn, count), bf16),
            pltpu.VMEM(key_up.shape, bf16),
            pltpu.VMEM(value_up.shape, bf16),
            pltpu.VMEM((128 * heads, 128), f32),
            pltpu.VMEM((both * heads, value_width), f32),
            pltpu.SemaphoreType.DMA((2, spans)),
            pltpu.SemaphoreType.DMA((3,)),
            pltpu.SemaphoreType.DMA((2, steps)),
            pltpu.SemaphoreType.DMA((2, steps)),
            pltpu.SemaphoreType.DMA((2, spans)),
            pltpu.SemaphoreType.DMA((2, spans)),
            pltpu.SemaphoreType.REGULAR,
        ],
        compiler_params=pltpu.CompilerParams(
            collective_id=0, has_side_effects=True, vmem_limit_bytes=40 * 1024 * 1024
        ),
    )(*(pltpu.with_memory_space_constraint(arg, pltpu.HBM) for arg in args))
    return pl.pallas_call(
        functools.partial(write_kernel, spans),
        out_shape=(
            jax.ShapeDtypeStruct((1, heads, width + turn, length), bf16),
            jax.ShapeDtypeStruct((1, length, heads, value_width), bf16),
        ),
        in_specs=[near] * 7,
        out_specs=[far] * 2,
        scratch_shapes=[
            pltpu.VMEM((heads, width + turn, count), bf16),
            pltpu.VMEM((count, heads, value_width), bf16),
            pltpu.VMEM((count * heads, value_width), f32),
            pltpu.SemaphoreType.DMA((2, spans)),
            pltpu.SemaphoreType.DMA((2,)),
        ],
        compiler_params=pltpu.CompilerParams(vmem_limit_bytes=16 * 1024 * 1024),
    )(*parts)


def solution(mesh):
    return jax.shard_map(
        shards,
        mesh=mesh,
        in_specs=(
            P("trial", ("span", "heads"), None),
            P("trial", ("span", "heads"), None),
            P(),
            P("trial", "heads", None),
            P("trial", "heads", None),
        ),
        out_specs=(
            P(("trial", "span"), "heads", None, None),
            P(("trial", "span"), None, "heads", None),
        ),
        check_vma=False,
    )
```

```python
import functools

import jax
import jax.numpy as jnp
from jax import lax
from jax.experimental import pallas as pl
from jax.experimental.pallas import tpu as pltpu
from jax.sharding import PartitionSpec as P

MESH = pl.DeviceIdType.MESH


def widen_rows(rows, rotary, key_up, value_up):
    wide_keys = jnp.einsum(
        "btr,rhk->bthk", rows, key_up, preferred_element_type=jnp.float32
    ).astype(jnp.bfloat16)
    shared = jnp.broadcast_to(rotary[:, :, None], wide_keys.shape[:3] + rotary.shape[2:])
    wide_values = jnp.einsum(
        "btr,rhk->bthk", rows, value_up, preferred_element_type=jnp.float32
    ).astype(jnp.bfloat16)
    return (jnp.concatenate([wide_keys, shared], axis=-1), wide_values)


def unit_rows(vectors, row_gain):
    return (
        vectors * lax.rsqrt(jnp.mean(vectors * vectors, axis=-1, keepdims=True) + 1e-06) * row_gain
    )


def plain_shards(latents, rotary_rows, latent_gain, key_up, value_up):
    rows_ready = unit_rows(latents.astype(jnp.float32), latent_gain).astype(jnp.bfloat16)

    def move(block):
        block = lax.all_to_all(block, "span", split_axis=0, concat_axis=1, tiled=True)
        block = block.reshape(block.shape[0], lax.axis_size("span"), -1, block.shape[2])
        block = lax.all_gather(block, "heads", axis=2, tiled=True)
        return block.reshape(block.shape[0], -1, block.shape[3])

    cache_keys, cache_values = widen_rows(move(rows_ready), move(rotary_rows), key_up, value_up)
    return (jnp.transpose(cache_keys, (0, 2, 3, 1)), cache_values)


def sibling(p):
    return p + 1 - 2 * lax.rem(p, 2)


def unit(raw, gain):
    sides, count, depth = raw.shape
    raw = raw.reshape(sides * count, depth).astype(jnp.float32)
    return unit_rows(raw, gain[...]).astype(jnp.bfloat16)


def expand_keys(ready, turned, key_wide, keys):
    heads, turn, count = keys.shape[0], turned.shape[1], turned.shape[2]
    width = keys.shape[1] - turn
    for h in range(heads):
        wide = lax.dot_general(
            key_wide[h * width:(h + 1) * width, :], ready,
            (((1,), (1,)), ((), ())), preferred_element_type=jnp.float32,
        )
        keys[h, :width, :] = wide.astype(jnp.bfloat16)
        for k in range(turned.shape[0]):
            keys[h, width:width + turn, k * count:(k + 1) * count] = turned[k]


def expand_values(ready, value_wide, flat, values):
    both, heads, width = values.shape
    for h in range(0, heads, 2):
        wide = jnp.dot(
            ready, value_wide[:, h * width:(h + 2) * width], preferred_element_type=jnp.float32
        )
        for k in range(2):
            flat[pl.ds(h + k, both, stride=heads), :] = wide[:, k * width:(k + 1) * width]
    values[...] = flat[pl.ds(0, both * heads), :].reshape(both, heads, width).astype(jnp.bfloat16)


def exchange_kernel(
    spans, lat, rot, far_gain, key_up, value_up, keys, values, rows_last, turned_last, key_wide, value_wide, gain,
    stage, stage_rot, rows, turned, raw_key, raw_value, flat, flat_out,
    load_sem, weight_sem, send_sem, recv_sem, pass_sem, land_sem, go_sem,
):
    me, side = lax.axis_index("span"), lax.axis_index("heads")
    other = 1 - side
    count, depth = lat.shape[1], lat.shape[2]
    heads, width = key_up.shape[1], key_up.shape[2]
    value_width = value_up.shape[2]
    turn = rot.shape[1]
    both = 2 * count

    targets, sources = [sibling(me)], [sibling(me)]
    for j in range(1, spans // 2):
        ahead, behind = lax.rem(me + 2 * j, spans), lax.rem(me + spans - 2 * j, spans)
        targets += [ahead, sibling(ahead)]
        sources += [behind, lax.rem(sibling(me) + spans - 2 * j, spans)]
    steps = len(targets)

    barrier = pltpu.get_barrier_semaphore()
    leader = spans - 1
    pl.semaphore_signal(barrier, inc=1, device_id={"heads": other}, device_id_type=MESH)

    @pl.when(me != leader)
    def _():
        pl.semaphore_signal(barrier, inc=1, device_id={"span": leader}, device_id_type=MESH)

    order = list(range(1, steps)) + [0]
    loads = {}
    own = (
        pltpu.make_async_copy(lat.at[me], rows.at[me, side], load_sem.at[0, steps]),
        pltpu.make_async_copy(rot.at[me], turned.at[me, side], load_sem.at[1, steps]),
    )
    for copy in own:
        copy.start()
    for i in order:
        loads[i] = (
            pltpu.make_async_copy(lat.at[targets[i]], stage.at[i], load_sem.at[0, i]),
            pltpu.make_async_copy(rot.at[targets[i]], stage_rot.at[i], load_sem.at[1, i]),
        )
        for copy in loads[i]:
            copy.start()
    weights = (
        pltpu.make_async_copy(key_up, raw_key, weight_sem.at[0]),
        pltpu.make_async_copy(value_up, raw_value, weight_sem.at[1]),
        pltpu.make_async_copy(far_gain, gain, weight_sem.at[2]),
    )
    for copy in weights:
        copy.start()

    @pl.when(me == leader)
    def _():
        pl.semaphore_wait(barrier, spans)
        for q in range(spans - 1):
            pl.semaphore_signal(go_sem, inc=1, device_id={"span": q}, device_id_type=MESH)

    @pl.when(me != leader)
    def _():
        pl.semaphore_wait(barrier, 1)

    def forward(q, i):
        made = []
        for k, held in enumerate((rows, turned)):
            made.append(pltpu.make_async_remote_copy(
                src_ref=(lat, rot)[k].at[me] if i == 0 else held.at[q, side], dst_ref=held.at[q, side],
                send_sem=pass_sem.at[k, i], recv_sem=land_sem.at[k, i],
                device_id={"heads": other}, device_id_type=MESH,
            ))
            made[-1].start()
        return made

    passed = [forward(me, 0)]

    @pl.when(me != leader)
    def _():
        pl.semaphore_wait(go_sem, 1)

    sent = {}
    for i in order:
        for copy in loads[i]:
            copy.wait()
        sent[i] = []
        for k, (held, land) in enumerate(((stage, rows), (stage_rot, turned))):
            sent[i].append(pltpu.make_async_remote_copy(
                src_ref=held.at[i], dst_ref=land.at[me, side],
                send_sem=send_sem.at[k, i], recv_sem=recv_sem.at[k, i],
                device_id={"span": targets[i]}, device_id_type=MESH,
            ))
            sent[i][-1].start()

    def hear(i):
        for k, (held, land) in enumerate(((stage, rows), (stage_rot, turned))):
            pltpu.make_async_remote_copy(
                src_ref=held.at[i], dst_ref=land.at[sources[i], side],
                send_sem=send_sem.at[k, i], recv_sem=recv_sem.at[k, i],
                device_id={"span": targets[i]}, device_id_type=MESH,
            ).wait_recv()
        passed.append(forward(sources[i], i + 1))

    def landed(q, i):
        for k, held in enumerate((rows, turned)):
            pltpu.make_async_remote_copy(
                src_ref=held.at[q, other], dst_ref=held.at[q, other],
                send_sem=pass_sem.at[k, i], recv_sem=land_sem.at[k, i],
                device_id={"heads": other}, device_id_type=MESH,
            ).wait_recv()

    def unravel(raw, size, put):
        piece = 128

        @pl.loop(0, depth // piece)
        def _(n):
            r = pl.multiple_of(n * piece, piece)
            part = raw[pl.ds(r, piece)].astype(jnp.float32)
            flat[pl.ds(0, piece * heads), :] = part.reshape(piece * heads, size)
            for h in range(heads):
                put(h, r, piece, flat[pl.ds(h, piece, stride=heads), :])

    def put_value(h, r, piece, block):
        value_wide[pl.ds(r, piece), h * value_width:(h + 1) * value_width] = block.astype(jnp.bfloat16)

    def put_key(h, r, piece, block):
        key_wide[h * width:(h + 1) * width, pl.ds(r, piece)] = block.T.astype(jnp.bfloat16)

    for copy in own:
        copy.wait()
    hear(0)
    for copy in weights:
        copy.wait()
    unravel(raw_key, width, put_key)
    unravel(raw_value, value_width, put_value)
    def finish(q):
        start = pl.multiple_of(q * both, both)
        expand_keys(
            unit(rows[q], gain), turned.at[q], key_wide, keys.at[:, :, pl.ds(start, both)]
        )
        expand_values(
            unit(rows[q], gain), value_wide, flat_out, values.at[pl.ds(start, both)]
        )

    for i in range(1, steps):
        hear(i)
        landed((me, *sources)[i - 1], i - 1)
        finish((me, *sources)[i - 1])
    last = sources[steps - 1]
    start = pl.multiple_of(last * both + side * count, count)
    half = pl.ds(side, 1)
    expand_keys(
        unit(rows[last, half], gain), turned.at[last, half], key_wide,
        keys.at[:, :, pl.ds(start, count)],
    )
    expand_values(
        unit(rows[last, half], gain), value_wide, flat_out, values.at[pl.ds(start, count)]
    )
    landed(sources[steps - 2], steps - 1)
    finish(sources[steps - 2])
    landed(last, steps)
    rows_last[...] = rows[last, pl.ds(other, 1)]
    turned_last[...] = turned[last, pl.ds(other, 1)]
    for pair in (*passed, *sent.values()):
        for copy in pair:
            copy.wait_send()


def write_kernel(
    spans, keys_part, values_part, rows_last, turned_last, key_wide, value_wide, gain,
    keys, values, keys_last, values_last, flat, sem, last_sem,
):
    me, side = lax.axis_index("span"), lax.axis_index("heads")
    count = values_last.shape[0]
    both = 2 * count
    order = [me, sibling(me)]
    for j in range(1, spans // 2):
        behind = lax.rem(me + spans - 2 * j, spans)
        order += [behind, lax.rem(sibling(me) + spans - 2 * j, spans)]
    last = order[-1] * both
    done = [pl.ds(pl.multiple_of(q * both, both), both) for q in order[:-1]]
    done.append(pl.ds(pl.multiple_of(last + side * count, count), count))
    copies = []
    for i, at in enumerate(done):
        copies += [
            pltpu.make_async_copy(keys_part.at[:, :, at], keys.at[0, :, :, at], sem.at[0, i]),
            pltpu.make_async_copy(values_part.at[at], values.at[0, at], sem.at[1, i]),
        ]
    for copy in copies:
        copy.start()
    at = pl.ds(pl.multiple_of(last + (1 - side) * count, count), count)
    ready = unit(rows_last[...], gain)
    expand_keys(ready, turned_last, key_wide, keys_last)
    copies.append(pltpu.make_async_copy(keys_last, keys.at[0, :, :, at], last_sem.at[0]))
    copies[-1].start()
    expand_values(ready, value_wide, flat, values_last)
    copies.append(pltpu.make_async_copy(values_last, values.at[0, at], last_sem.at[1]))
    copies[-1].start()
    for copy in copies:
        copy.wait()


def shards(latents, rotary_rows, latent_gain, key_up, value_up):
    spans, sides = lax.axis_size("span"), lax.axis_size("heads")
    _, count, depth = latents.shape
    turn = rotary_rows.shape[2]
    heads, width, value_width = key_up.shape[1], key_up.shape[2], value_up.shape[2]
    if (
        latents.shape[0] != spans or spans % 2 or sides != 2 or count % 128 or depth % 128
        or heads % 8 or width != 128 or value_width != 128 or turn % 16
    ):
        return plain_shards(latents, rotary_rows, latent_gain, key_up, value_up)
    length, both = spans * sides * count, sides * count
    steps = spans - 1
    bf16, f32 = jnp.bfloat16, jnp.float32
    near = pl.BlockSpec(memory_space=pltpu.VMEM)
    far = pl.BlockSpec(memory_space=pltpu.HBM)
    args = (latents, jnp.swapaxes(rotary_rows, 1, 2), latent_gain[None], key_up, value_up)
    parts = pl.pallas_call(
        functools.partial(exchange_kernel, spans),
        out_shape=(
            pltpu.VMEM((heads, width + turn, length), bf16),
            pltpu.VMEM((length, heads, value_width), bf16),
            pltpu.VMEM((1, count, depth), bf16),
            pltpu.VMEM((1, turn, count), bf16),
            pltpu.VMEM((heads * width, depth), bf16),
            pltpu.VMEM((depth, heads * value_width), bf16),
            pltpu.VMEM((1, depth), f32),
        ),
        in_specs=[far] * 5,
        out_specs=[near] * 7,
        scratch_shapes=[
            pltpu.VMEM((steps, count, depth), bf16),
            pltpu.VMEM((steps, turn, count), bf16),
            pltpu.VMEM((spans, sides, count, depth), bf16),
            pltpu.VMEM((spans, sides, turn, count), bf16),
            pltpu.VMEM(key_up.shape, bf16),
            pltpu.VMEM(value_up.shape, bf16),
            pltpu.VMEM((128 * heads, 128), f32),
            pltpu.VMEM((both * heads, value_width), f32),
            pltpu.SemaphoreType.DMA((2, spans)),
            pltpu.SemaphoreType.DMA((3,)),
            pltpu.SemaphoreType.DMA((2, steps)),
            pltpu.SemaphoreType.DMA((2, steps)),
            pltpu.SemaphoreType.DMA((2, spans)),
            pltpu.SemaphoreType.DMA((2, spans)),
            pltpu.SemaphoreType.REGULAR,
        ],
        compiler_params=pltpu.CompilerParams(
            collective_id=0, has_side_effects=True, vmem_limit_bytes=40 * 1024 * 1024
        ),
    )(*(pltpu.with_memory_space_constraint(arg, pltpu.HBM) for arg in args))
    return pl.pallas_call(
        functools.partial(write_kernel, spans),
        out_shape=(
            jax.ShapeDtypeStruct((1, heads, width + turn, length), bf16),
            jax.ShapeDtypeStruct((1, length, heads, value_width), bf16),
        ),
        in_specs=[near] * 7,
        out_specs=[far] * 2,
        scratch_shapes=[
            pltpu.VMEM((heads, width + turn, count), bf16),
            pltpu.VMEM((count, heads, value_width), bf16),
            pltpu.VMEM((count * heads, value_width), f32),
            pltpu.SemaphoreType.DMA((2, spans)),
            pltpu.SemaphoreType.DMA((2,)),
        ],
        compiler_params=pltpu.CompilerParams(vmem_limit_bytes=16 * 1024 * 1024),
    )(*parts)


def solution(mesh):
    return jax.shard_map(
        shards,
        mesh=mesh,
        in_specs=(
            P("trial", ("span", "heads"), None),
            P("trial", ("span", "heads"), None),
            P(),
            P("trial", "heads", None),
            P("trial", "heads", None),
        ),
        out_specs=(
            P(("trial", "span"), "heads", None, None),
            P(("trial", "span"), None, "heads", None),
        ),
        check_vma=False,
    )
```

```python
import functools

import jax
import jax.numpy as jnp
from jax import lax
from jax.experimental import pallas as pl
from jax.experimental.pallas import tpu as pltpu
from jax.sharding import PartitionSpec as P

MESH = pl.DeviceIdType.MESH


def widen_rows(rows, rotary, key_up, value_up):
    wide_keys = jnp.einsum(
        "btr,rhk->bthk", rows, key_up, preferred_element_type=jnp.float32
    ).astype(jnp.bfloat16)
    shared = jnp.broadcast_to(rotary[:, :, None], wide_keys.shape[:3] + rotary.shape[2:])
    wide_values = jnp.einsum(
        "btr,rhk->bthk", rows, value_up, preferred_element_type=jnp.float32
    ).astype(jnp.bfloat16)
    return (jnp.concatenate([wide_keys, shared], axis=-1), wide_values)


def unit_rows(vectors, row_gain):
    return (
        vectors * lax.rsqrt(jnp.mean(vectors * vectors, axis=-1, keepdims=True) + 1e-06) * row_gain
    )


def plain_shards(latents, rotary_rows, latent_gain, key_up, value_up):
    rows_ready = unit_rows(latents.astype(jnp.float32), latent_gain).astype(jnp.bfloat16)

    def move(block):
        block = lax.all_to_all(block, "span", split_axis=0, concat_axis=1, tiled=True)
        block = block.reshape(block.shape[0], lax.axis_size("span"), -1, block.shape[2])
        block = lax.all_gather(block, "heads", axis=2, tiled=True)
        return block.reshape(block.shape[0], -1, block.shape[3])

    cache_keys, cache_values = widen_rows(move(rows_ready), move(rotary_rows), key_up, value_up)
    return (jnp.transpose(cache_keys, (0, 2, 3, 1)), cache_values)


def sibling(p):
    return p + 1 - 2 * lax.rem(p, 2)


def unit(raw, gain):
    sides, count, depth = raw.shape
    raw = raw.reshape(sides * count, depth).astype(jnp.float32)
    return unit_rows(raw, gain[...]).astype(jnp.bfloat16)


def expand_keys(ready, turned, key_wide, keys):
    heads, turn, count = keys.shape[0], turned.shape[1], turned.shape[2]
    width = keys.shape[1] - turn
    for h in range(heads):
        wide = lax.dot_general(
            key_wide[h * width:(h + 1) * width, :], ready,
            (((1,), (1,)), ((), ())), preferred_element_type=jnp.float32,
        )
        keys[h, :width, :] = wide.astype(jnp.bfloat16)
        for k in range(turned.shape[0]):
            keys[h, width:width + turn, k * count:(k + 1) * count] = turned[k]


def expand_values(ready, value_wide, flat, values):
    both, heads, width = values.shape
    for h in range(0, heads, 2):
        wide = jnp.dot(
            ready, value_wide[:, h * width:(h + 2) * width], preferred_element_type=jnp.float32
        )
        for k in range(2):
            flat[pl.ds(h + k, both, stride=heads), :] = wide[:, k * width:(k + 1) * width]
    values[...] = flat[pl.ds(0, both * heads), :].reshape(both, heads, width).astype(jnp.bfloat16)


def exchange_kernel(
    spans, lat, rot, far_gain, key_up, value_up, keys, values, rows_last, turned_last, key_wide, value_wide, gain,
    rows, turned, raw_key, raw_value, flat, flat_out,
    load_sem, weight_sem, send_sem, recv_sem, pass_sem, land_sem, go_sem,
):
    me, side = lax.axis_index("span"), lax.axis_index("heads")
    other = 1 - side
    count, depth = lat.shape[1], lat.shape[2]
    heads, width = key_up.shape[1], key_up.shape[2]
    value_width = value_up.shape[2]
    turn = rot.shape[1]
    both = 2 * count

    targets, sources = [sibling(me)], [sibling(me)]
    for j in range(1, spans // 2):
        ahead, behind = lax.rem(me + 2 * j, spans), lax.rem(me + spans - 2 * j, spans)
        targets += [ahead, sibling(ahead)]
        sources += [behind, lax.rem(sibling(me) + spans - 2 * j, spans)]
    steps = len(targets)

    barrier = pltpu.get_barrier_semaphore()
    leader = spans - 1
    pl.semaphore_signal(barrier, inc=1, device_id={"heads": other}, device_id_type=MESH)

    @pl.when(me != leader)
    def _():
        pl.semaphore_signal(barrier, inc=1, device_id={"span": leader}, device_id_type=MESH)

    order = list(range(1, steps)) + [0]
    own = (
        pltpu.make_async_copy(lat.at[me], rows.at[me, side], load_sem.at[0]),
        pltpu.make_async_copy(rot.at[me], turned.at[me, side], load_sem.at[1]),
    )
    for copy in own:
        copy.start()
    weights = (
        pltpu.make_async_copy(key_up, raw_key, weight_sem.at[0]),
        pltpu.make_async_copy(value_up, raw_value, weight_sem.at[1]),
        pltpu.make_async_copy(far_gain, gain, weight_sem.at[2]),
    )
    for copy in weights:
        copy.start()

    @pl.when(me == leader)
    def _():
        pl.semaphore_wait(barrier, spans)
        for q in range(spans - 1):
            pl.semaphore_signal(go_sem, inc=1, device_id={"span": q}, device_id_type=MESH)

    @pl.when(me != leader)
    def _():
        pl.semaphore_wait(barrier, 1)

    def forward(q, i):
        made = []
        for k, held in enumerate((rows, turned)):
            made.append(pltpu.make_async_remote_copy(
                src_ref=(lat, rot)[k].at[me] if i == 0 else held.at[q, side], dst_ref=held.at[q, side],
                send_sem=pass_sem.at[k, i], recv_sem=land_sem.at[k, i],
                device_id={"heads": other}, device_id_type=MESH,
            ))
            made[-1].start()
        return made

    passed = [forward(me, 0)]

    @pl.when(me != leader)
    def _():
        pl.semaphore_wait(go_sem, 1)

    sent = {}
    for i in order:
        sent[i] = []
        for k, (held, land) in enumerate(((lat, rows), (rot, turned))):
            sent[i].append(pltpu.make_async_remote_copy(
                src_ref=held.at[targets[i]], dst_ref=land.at[me, side],
                send_sem=send_sem.at[k, i], recv_sem=recv_sem.at[k, i],
                device_id={"span": targets[i]}, device_id_type=MESH,
            ))
            sent[i][-1].start()

    def hear(i):
        for k, (held, land) in enumerate(((lat, rows), (rot, turned))):
            pltpu.make_async_remote_copy(
                src_ref=held.at[targets[i]], dst_ref=land.at[sources[i], side],
                send_sem=send_sem.at[k, i], recv_sem=recv_sem.at[k, i],
                device_id={"span": targets[i]}, device_id_type=MESH,
            ).wait_recv()
        passed.append(forward(sources[i], i + 1))

    def landed(q, i):
        for k, held in enumerate((rows, turned)):
            pltpu.make_async_remote_copy(
                src_ref=held.at[q, other], dst_ref=held.at[q, other],
                send_sem=pass_sem.at[k, i], recv_sem=land_sem.at[k, i],
                device_id={"heads": other}, device_id_type=MESH,
            ).wait_recv()

    def unravel(raw, size, put):
        piece = 128

        @pl.loop(0, depth // piece)
        def _(n):
            r = pl.multiple_of(n * piece, piece)
            part = raw[pl.ds(r, piece)].astype(jnp.float32)
            flat[pl.ds(0, piece * heads), :] = part.reshape(piece * heads, size)
            for h in range(heads):
                put(h, r, piece, flat[pl.ds(h, piece, stride=heads), :])

    def put_value(h, r, piece, block):
        value_wide[pl.ds(r, piece), h * value_width:(h + 1) * value_width] = block.astype(jnp.bfloat16)

    def put_key(h, r, piece, block):
        key_wide[h * width:(h + 1) * width, pl.ds(r, piece)] = block.T.astype(jnp.bfloat16)

    for copy in own:
        copy.wait()
    hear(0)
    for copy in weights:
        copy.wait()
    unravel(raw_key, width, put_key)
    unravel(raw_value, value_width, put_value)
    def finish(q):
        start = pl.multiple_of(q * both, both)
        expand_keys(
            unit(rows[q], gain), turned.at[q], key_wide, keys.at[:, :, pl.ds(start, both)]
        )
        expand_values(
            unit(rows[q], gain), value_wide, flat_out, values.at[pl.ds(start, both)]
        )

    for i in range(1, steps):
        hear(i)
        landed((me, *sources)[i - 1], i - 1)
        finish((me, *sources)[i - 1])
    last = sources[steps - 1]
    start = pl.multiple_of(last * both + side * count, count)
    half = pl.ds(side, 1)
    expand_keys(
        unit(rows[last, half], gain), turned.at[last, half], key_wide,
        keys.at[:, :, pl.ds(start, count)],
    )
    expand_values(
        unit(rows[last, half], gain), value_wide, flat_out, values.at[pl.ds(start, count)]
    )
    landed(sources[steps - 2], steps - 1)
    finish(sources[steps - 2])
    landed(last, steps)
    rows_last[...] = rows[last, pl.ds(other, 1)]
    turned_last[...] = turned[last, pl.ds(other, 1)]
    for pair in (*passed, *sent.values()):
        for copy in pair:
            copy.wait_send()


def write_kernel(
    spans, keys_part, values_part, rows_last, turned_last, key_wide, value_wide, gain,
    keys, values, keys_last, values_last, flat, sem, last_sem,
):
    me, side = lax.axis_index("span"), lax.axis_index("heads")
    count = values_last.shape[0]
    both = 2 * count
    order = [me, sibling(me)]
    for j in range(1, spans // 2):
        behind = lax.rem(me + spans - 2 * j, spans)
        order += [behind, lax.rem(sibling(me) + spans - 2 * j, spans)]
    last = order[-1] * both
    done = [pl.ds(pl.multiple_of(q * both, both), both) for q in order[:-1]]
    done.append(pl.ds(pl.multiple_of(last + side * count, count), count))
    copies = []
    for i, at in enumerate(done):
        copies += [
            pltpu.make_async_copy(keys_part.at[:, :, at], keys.at[0, :, :, at], sem.at[0, i]),
            pltpu.make_async_copy(values_part.at[at], values.at[0, at], sem.at[1, i]),
        ]
    for copy in copies:
        copy.start()
    at = pl.ds(pl.multiple_of(last + (1 - side) * count, count), count)
    ends = (
        pltpu.make_async_copy(keys_last, keys.at[0, :, :, at], last_sem.at[0]),
        pltpu.make_async_copy(values_last, values.at[0, at], last_sem.at[1]),
    )

    @pl.when(me >= 0)
    def _():
        ready = unit(rows_last[...], gain)
        expand_keys(ready, turned_last, key_wide, keys_last)
        ends[0].start()
        expand_values(ready, value_wide, flat, values_last)
        ends[1].start()

    for copy in (*copies, *ends):
        copy.wait()


def shards(latents, rotary_rows, latent_gain, key_up, value_up):
    spans, sides = lax.axis_size("span"), lax.axis_size("heads")
    _, count, depth = latents.shape
    turn = rotary_rows.shape[2]
    heads, width, value_width = key_up.shape[1], key_up.shape[2], value_up.shape[2]
    if (
        latents.shape[0] != spans or spans % 2 or sides != 2 or count % 128 or depth % 128
        or heads % 8 or width != 128 or value_width != 128 or turn % 16
    ):
        return plain_shards(latents, rotary_rows, latent_gain, key_up, value_up)
    length, both = spans * sides * count, sides * count
    steps = spans - 1
    bf16, f32 = jnp.bfloat16, jnp.float32
    near = pl.BlockSpec(memory_space=pltpu.VMEM)
    far = pl.BlockSpec(memory_space=pltpu.HBM)
    args = (latents, jnp.swapaxes(rotary_rows, 1, 2), latent_gain[None], key_up, value_up)
    parts = pl.pallas_call(
        functools.partial(exchange_kernel, spans),
        out_shape=(
            pltpu.VMEM((heads, width + turn, length), bf16),
            pltpu.VMEM((length, heads, value_width), bf16),
            pltpu.VMEM((1, count, depth), bf16),
            pltpu.VMEM((1, turn, count), bf16),
            pltpu.VMEM((heads * width, depth), bf16),
            pltpu.VMEM((depth, heads * value_width), bf16),
            pltpu.VMEM((1, depth), f32),
        ),
        in_specs=[far] * 5,
        out_specs=[near] * 7,
        scratch_shapes=[
            pltpu.VMEM((spans, sides, count, depth), bf16),
            pltpu.VMEM((spans, sides, turn, count), bf16),
            pltpu.VMEM(key_up.shape, bf16),
            pltpu.VMEM(value_up.shape, bf16),
            pltpu.VMEM((128 * heads, 128), f32),
            pltpu.VMEM((both * heads, value_width), f32),
            pltpu.SemaphoreType.DMA((2,)),
            pltpu.SemaphoreType.DMA((3,)),
            pltpu.SemaphoreType.DMA((2, steps)),
            pltpu.SemaphoreType.DMA((2, steps)),
            pltpu.SemaphoreType.DMA((2, spans)),
            pltpu.SemaphoreType.DMA((2, spans)),
            pltpu.SemaphoreType.REGULAR,
        ],
        compiler_params=pltpu.CompilerParams(
            collective_id=0, has_side_effects=True, vmem_limit_bytes=40 * 1024 * 1024
        ),
    )(*(pltpu.with_memory_space_constraint(arg, pltpu.HBM) for arg in args))
    return pl.pallas_call(
        functools.partial(write_kernel, spans),
        out_shape=(
            jax.ShapeDtypeStruct((1, heads, width + turn, length), bf16),
            jax.ShapeDtypeStruct((1, length, heads, value_width), bf16),
        ),
        in_specs=[near] * 7,
        out_specs=[far] * 2,
        scratch_shapes=[
            pltpu.VMEM((heads, width + turn, count), bf16),
            pltpu.VMEM((count, heads, value_width), bf16),
            pltpu.VMEM((count * heads, value_width), f32),
            pltpu.SemaphoreType.DMA((2, spans)),
            pltpu.SemaphoreType.DMA((2,)),
        ],
        compiler_params=pltpu.CompilerParams(vmem_limit_bytes=16 * 1024 * 1024),
    )(*parts)


def solution(mesh):
    return jax.shard_map(
        shards,
        mesh=mesh,
        in_specs=(
            P("trial", ("span", "heads"), None),
            P("trial", ("span", "heads"), None),
            P(),
            P("trial", "heads", None),
            P("trial", "heads", None),
        ),
        out_specs=(
            P(("trial", "span"), "heads", None, None),
            P(("trial", "span"), None, "heads", None),
        ),
        check_vma=False,
    )
```

```python
import functools

import jax
import jax.numpy as jnp
from jax import lax
from jax.experimental import pallas as pl
from jax.experimental.pallas import tpu as pltpu
from jax.sharding import PartitionSpec as P

MESH = pl.DeviceIdType.MESH


def widen_rows(rows, rotary, key_up, value_up):
    wide_keys = jnp.einsum(
        "btr,rhk->bthk", rows, key_up, preferred_element_type=jnp.float32
    ).astype(jnp.bfloat16)
    shared = jnp.broadcast_to(rotary[:, :, None], wide_keys.shape[:3] + rotary.shape[2:])
    wide_values = jnp.einsum(
        "btr,rhk->bthk", rows, value_up, preferred_element_type=jnp.float32
    ).astype(jnp.bfloat16)
    return (jnp.concatenate([wide_keys, shared], axis=-1), wide_values)


def unit_rows(vectors, row_gain):
    return (
        vectors * lax.rsqrt(jnp.mean(vectors * vectors, axis=-1, keepdims=True) + 1e-06) * row_gain
    )


def plain_shards(latents, rotary_rows, latent_gain, key_up, value_up):
    rows_ready = unit_rows(latents.astype(jnp.float32), latent_gain).astype(jnp.bfloat16)

    def move(block):
        block = lax.all_to_all(block, "span", split_axis=0, concat_axis=1, tiled=True)
        block = block.reshape(block.shape[0], lax.axis_size("span"), -1, block.shape[2])
        block = lax.all_gather(block, "heads", axis=2, tiled=True)
        return block.reshape(block.shape[0], -1, block.shape[3])

    cache_keys, cache_values = widen_rows(move(rows_ready), move(rotary_rows), key_up, value_up)
    return (jnp.transpose(cache_keys, (0, 2, 3, 1)), cache_values)


def sibling(p):
    return p + 1 - 2 * lax.rem(p, 2)


def unit(raw, gain):
    sides, count, depth = raw.shape
    raw = raw.reshape(sides * count, depth).astype(jnp.float32)
    return unit_rows(raw, gain[...]).astype(jnp.bfloat16)


def expand_keys(ready, turned, key_wide, keys):
    heads, turn, count = keys.shape[0], turned.shape[1], turned.shape[2]
    width = keys.shape[1] - turn
    for h in range(heads):
        wide = lax.dot_general(
            key_wide[h * width:(h + 1) * width, :], ready,
            (((1,), (1,)), ((), ())), preferred_element_type=jnp.float32,
        )
        keys[h, :width, :] = wide.astype(jnp.bfloat16)
        for k in range(turned.shape[0]):
            keys[h, width:width + turn, k * count:(k + 1) * count] = turned[k]


def expand_values(ready, value_wide, flat, values):
    both, heads, width = values.shape
    for h in range(0, heads, 2):
        wide = jnp.dot(
            ready, value_wide[:, h * width:(h + 2) * width], preferred_element_type=jnp.float32
        )
        for k in range(2):
            flat[pl.ds(h + k, both, stride=heads), :] = wide[:, k * width:(k + 1) * width]
    values[...] = flat[pl.ds(0, both * heads), :].reshape(both, heads, width).astype(jnp.bfloat16)


def exchange_kernel(
    spans, lat, rot, far_gain, key_up, value_up, keys, values, rows_last, turned_last, key_wide, value_wide, gain,
    rows, turned, raw_key, raw_value, flat, flat_out,
    load_sem, weight_sem, send_sem, recv_sem, pass_sem, land_sem, chip_sem, go_sem,
):
    me, side = lax.axis_index("span"), lax.axis_index("heads")
    other = 1 - side
    count, depth = lat.shape[1], lat.shape[2]
    heads, width = key_up.shape[1], key_up.shape[2]
    value_width = value_up.shape[2]
    turn = rot.shape[1]
    both = 2 * count

    targets, sources = [sibling(me)], [sibling(me)]
    for j in range(1, spans // 2):
        ahead, behind = lax.rem(me + 2 * j, spans), lax.rem(me + spans - 2 * j, spans)
        targets += [ahead, sibling(ahead)]
        sources += [behind, lax.rem(sibling(me) + spans - 2 * j, spans)]
    steps = len(targets)

    barrier = pltpu.get_barrier_semaphore()
    leader = spans - 1
    pl.semaphore_signal(barrier, inc=1, device_id={"heads": other}, device_id_type=MESH)

    odd = lax.rem(me, 2)

    @pl.when(odd == 0)
    def _():
        pl.semaphore_signal(barrier, inc=1, device_id={"span": me + 1}, device_id_type=MESH)

    order = list(range(steps))
    own = (
        pltpu.make_async_copy(lat.at[me], rows.at[me, side], load_sem.at[0]),
        pltpu.make_async_copy(rot.at[me], turned.at[me, side], load_sem.at[1]),
    )
    for copy in own:
        copy.start()
    weights = (
        pltpu.make_async_copy(key_up, raw_key, weight_sem.at[0]),
        pltpu.make_async_copy(value_up, raw_value, weight_sem.at[1]),
        pltpu.make_async_copy(far_gain, gain, weight_sem.at[2]),
    )
    for copy in weights:
        copy.start()

    @pl.when(odd == 0)
    def _():
        pl.semaphore_wait(barrier, 1)

    @pl.when((odd == 1) & (me != leader))
    def _():
        pl.semaphore_wait(barrier, 2)
        pl.semaphore_signal(chip_sem, inc=1, device_id={"span": me - 1}, device_id_type=MESH)
        pl.semaphore_signal(barrier, inc=1, device_id={"span": leader}, device_id_type=MESH)

    @pl.when(me == leader)
    def _():
        pl.semaphore_wait(barrier, 1 + spans // 2)
        pl.semaphore_signal(chip_sem, inc=1, device_id={"span": leader - 1}, device_id_type=MESH)
        for q in range(spans - 1):
            pl.semaphore_signal(go_sem, inc=1, device_id={"span": q}, device_id_type=MESH)

    def forward(q, i):
        made = []
        for k, held in enumerate((rows, turned)):
            made.append(pltpu.make_async_remote_copy(
                src_ref=(lat, rot)[k].at[me] if i == 0 else held.at[q, side], dst_ref=held.at[q, side],
                send_sem=pass_sem.at[k, i], recv_sem=land_sem.at[k, i],
                device_id={"heads": other}, device_id_type=MESH,
            ))
            made[-1].start()
        return made

    passed = [forward(me, 0)]

    @pl.when(odd == 0)
    def _():
        pl.semaphore_wait(chip_sem, 1)

    sent = {}
    for i in order:
        if i == 1:

            @pl.when(me != leader)
            def _():
                pl.semaphore_wait(go_sem, 1)

        sent[i] = []
        for k, (held, land) in enumerate(((lat, rows), (rot, turned))):
            sent[i].append(pltpu.make_async_remote_copy(
                src_ref=held.at[targets[i]], dst_ref=land.at[me, side],
                send_sem=send_sem.at[k, i], recv_sem=recv_sem.at[k, i],
                device_id={"span": targets[i]}, device_id_type=MESH,
            ))
            sent[i][-1].start()

    def hear(i):
        for k, (held, land) in enumerate(((lat, rows), (rot, turned))):
            pltpu.make_async_remote_copy(
                src_ref=held.at[targets[i]], dst_ref=land.at[sources[i], side],
                send_sem=send_sem.at[k, i], recv_sem=recv_sem.at[k, i],
                device_id={"span": targets[i]}, device_id_type=MESH,
            ).wait_recv()
        passed.append(forward(sources[i], i + 1))

    def landed(q, i):
        for k, held in enumerate((rows, turned)):
            pltpu.make_async_remote_copy(
                src_ref=held.at[q, other], dst_ref=held.at[q, other],
                send_sem=pass_sem.at[k, i], recv_sem=land_sem.at[k, i],
                device_id={"heads": other}, device_id_type=MESH,
            ).wait_recv()

    def unravel(raw, size, put):
        piece = 128

        @pl.loop(0, depth // piece)
        def _(n):
            r = pl.multiple_of(n * piece, piece)
            part = raw[pl.ds(r, piece)].astype(jnp.float32)
            flat[pl.ds(0, piece * heads), :] = part.reshape(piece * heads, size)
            for h in range(heads):
                put(h, r, piece, flat[pl.ds(h, piece, stride=heads), :])

    def put_value(h, r, piece, block):
        value_wide[pl.ds(r, piece), h * value_width:(h + 1) * value_width] = block.astype(jnp.bfloat16)

    def put_key(h, r, piece, block):
        key_wide[h * width:(h + 1) * width, pl.ds(r, piece)] = block.T.astype(jnp.bfloat16)

    for copy in own:
        copy.wait()
    hear(0)
    for copy in weights:
        copy.wait()
    unravel(raw_key, width, put_key)
    unravel(raw_value, value_width, put_value)
    def finish(q):
        start = pl.multiple_of(q * both, both)
        expand_keys(
            unit(rows[q], gain), turned.at[q], key_wide, keys.at[:, :, pl.ds(start, both)]
        )
        expand_values(
            unit(rows[q], gain), value_wide, flat_out, values.at[pl.ds(start, both)]
        )

    for i in range(1, steps):
        hear(i)
        landed((me, *sources)[i - 1], i - 1)
        finish((me, *sources)[i - 1])
    last = sources[steps - 1]
    start = pl.multiple_of(last * both + side * count, count)
    half = pl.ds(side, 1)
    expand_keys(
        unit(rows[last, half], gain), turned.at[last, half], key_wide,
        keys.at[:, :, pl.ds(start, count)],
    )
    expand_values(
        unit(rows[last, half], gain), value_wide, flat_out, values.at[pl.ds(start, count)]
    )
    landed(sources[steps - 2], steps - 1)
    finish(sources[steps - 2])
    landed(last, steps)
    rows_last[...] = rows[last, pl.ds(other, 1)]
    turned_last[...] = turned[last, pl.ds(other, 1)]
    for pair in (*passed, *sent.values()):
        for copy in pair:
            copy.wait_send()


def write_kernel(
    spans, keys_part, values_part, rows_last, turned_last, key_wide, value_wide, gain,
    keys, values, keys_last, values_last, flat, sem, last_sem,
):
    me, side = lax.axis_index("span"), lax.axis_index("heads")
    count = values_last.shape[0]
    both = 2 * count
    order = [me, sibling(me)]
    for j in range(1, spans // 2):
        behind = lax.rem(me + spans - 2 * j, spans)
        order += [behind, lax.rem(sibling(me) + spans - 2 * j, spans)]
    last = order[-1] * both
    done = [pl.ds(pl.multiple_of(q * both, both), both) for q in order[:-1]]
    done.append(pl.ds(pl.multiple_of(last + side * count, count), count))
    copies = []
    for i, at in enumerate(done):
        copies += [
            pltpu.make_async_copy(keys_part.at[:, :, at], keys.at[0, :, :, at], sem.at[0, i]),
            pltpu.make_async_copy(values_part.at[at], values.at[0, at], sem.at[1, i]),
        ]
    for copy in copies:
        copy.start()
    at = pl.ds(pl.multiple_of(last + (1 - side) * count, count), count)
    ends = (
        pltpu.make_async_copy(keys_last, keys.at[0, :, :, at], last_sem.at[0]),
        pltpu.make_async_copy(values_last, values.at[0, at], last_sem.at[1]),
    )

    @pl.when(me >= 0)
    def _():
        ready = unit(rows_last[...], gain)
        expand_keys(ready, turned_last, key_wide, keys_last)
        ends[0].start()
        expand_values(ready, value_wide, flat, values_last)
        ends[1].start()

    for copy in (*copies, *ends):
        copy.wait()


def shards(latents, rotary_rows, latent_gain, key_up, value_up):
    spans, sides = lax.axis_size("span"), lax.axis_size("heads")
    _, count, depth = latents.shape
    turn = rotary_rows.shape[2]
    heads, width, value_width = key_up.shape[1], key_up.shape[2], value_up.shape[2]
    if (
        latents.shape[0] != spans or spans % 2 or spans < 4 or sides != 2 or count % 128 or depth % 128
        or heads % 8 or width != 128 or value_width != 128 or turn % 16
    ):
        return plain_shards(latents, rotary_rows, latent_gain, key_up, value_up)
    length, both = spans * sides * count, sides * count
    steps = spans - 1
    bf16, f32 = jnp.bfloat16, jnp.float32
    near = pl.BlockSpec(memory_space=pltpu.VMEM)
    far = pl.BlockSpec(memory_space=pltpu.HBM)
    args = (latents, jnp.swapaxes(rotary_rows, 1, 2), latent_gain[None], key_up, value_up)
    parts = pl.pallas_call(
        functools.partial(exchange_kernel, spans),
        out_shape=(
            pltpu.VMEM((heads, width + turn, length), bf16),
            pltpu.VMEM((length, heads, value_width), bf16),
            pltpu.VMEM((1, count, depth), bf16),
            pltpu.VMEM((1, turn, count), bf16),
            pltpu.VMEM((heads * width, depth), bf16),
            pltpu.VMEM((depth, heads * value_width), bf16),
            pltpu.VMEM((1, depth), f32),
        ),
        in_specs=[far] * 5,
        out_specs=[near] * 7,
        scratch_shapes=[
            pltpu.VMEM((spans, sides, count, depth), bf16),
            pltpu.VMEM((spans, sides, turn, count), bf16),
            pltpu.VMEM(key_up.shape, bf16),
            pltpu.VMEM(value_up.shape, bf16),
            pltpu.VMEM((128 * heads, 128), f32),
            pltpu.VMEM((both * heads, value_width), f32),
            pltpu.SemaphoreType.DMA((2,)),
            pltpu.SemaphoreType.DMA((3,)),
            pltpu.SemaphoreType.DMA((2, steps)),
            pltpu.SemaphoreType.DMA((2, steps)),
            pltpu.SemaphoreType.DMA((2, spans)),
            pltpu.SemaphoreType.DMA((2, spans)),
            pltpu.SemaphoreType.REGULAR,
            pltpu.SemaphoreType.REGULAR,
        ],
        compiler_params=pltpu.CompilerParams(
            collective_id=0, has_side_effects=True, vmem_limit_bytes=40 * 1024 * 1024
        ),
    )(*(pltpu.with_memory_space_constraint(arg, pltpu.HBM) for arg in args))
    return pl.pallas_call(
        functools.partial(write_kernel, spans),
        out_shape=(
            jax.ShapeDtypeStruct((1, heads, width + turn, length), bf16),
            jax.ShapeDtypeStruct((1, length, heads, value_width), bf16),
        ),
        in_specs=[near] * 7,
        out_specs=[far] * 2,
        scratch_shapes=[
            pltpu.VMEM((heads, width + turn, count), bf16),
            pltpu.VMEM((count, heads, value_width), bf16),
            pltpu.VMEM((count * heads, value_width), f32),
            pltpu.SemaphoreType.DMA((2, spans)),
            pltpu.SemaphoreType.DMA((2,)),
        ],
        compiler_params=pltpu.CompilerParams(vmem_limit_bytes=16 * 1024 * 1024),
    )(*parts)


def solution(mesh):
    return jax.shard_map(
        shards,
        mesh=mesh,
        in_specs=(
            P("trial", ("span", "heads"), None),
            P("trial", ("span", "heads"), None),
            P(),
            P("trial", "heads", None),
            P("trial", "heads", None),
        ),
        out_specs=(
            P(("trial", "span"), "heads", None, None),
            P(("trial", "span"), None, "heads", None),
        ),
        check_vma=False,
    )
```
